256 devices in a mesh: pts: 32 (over z, y_lo, core), grp: 8 (over y_hi, x).
Axes of the slice: x: 4, y: 4 (y_hi: 2, y_lo: 2; y = y_hi * 2 + y_lo), z: 8, core: 2. Of those that a mesh axis runs over, the one named last changes fastest.
Arguments:
- occ_orbitals: bfloat16 [8192, 1024], P('pts'), may hold values from -0.1875 to 0.1875
- virt_orbitals: bfloat16 [8192, 1024], P('pts'), may hold values from -0.1875 to 0.1875
- columns: bfloat16 [8192, 512], P('pts'), may hold values from -6 to 6
- occ_energies: float32 [1024], replicated, may hold values from -3 to -0.1
- vir_energies: float32 [1024], replicated, may hold values from 0.1 to 3
- tau_index: int32 [8], replicated, may hold values from 0 to 15, as said below
- quad_weights: float32 [8], replicated, may hold values from 0.05 to 0.5
- frequencies: float32 [2], replicated, may hold values from 0.2 to 2
- distance_kept: int32 [32], replicated, may hold values 0 or 1
Outputs:
- response: float32 [2, 512, 8192], P(None, 'grp', 'pts')
The draws below stay inside these ranges and needn't reach their ends.
Inputs may be any that keep to these rules, and one draw needn't show every extreme that they name: `tau_index`: all entries differ; 0 and 15 are always among them.
All inputs are finite; a program needn't handle non-finite values.
Results may differ from the reference program's by a relative error of at most 0.0026.
Values may be sent and summed in bfloat16 or wider, within the bound.
No kernel may reach another device: no remote copies, remote signals or barrier semaphores. Data moves between devices by JAX's collectives and lax.ppermute only.
A program may use at most 64 MiB of HBM per device.

```python
import math
import jax
import jax.numpy as jnp
from jax import lax

NOCC = 1024
NVIR = 1024
BP = 256
NCOL = 512
NTAU = 8
NGRID = 16
NFREQ = 2
NP = 8192
N_PTS = 32


def draw_tau_index(key, part):
    inner_key = jax.random.fold_in(key, 11)
    order_key = jax.random.fold_in(key, 23)
    middle = jax.random.permutation(inner_key, NGRID - 2)[:NTAU - 2].astype(jnp.int32) + 1
    chosen = jnp.concatenate([jnp.zeros((1,), jnp.int32), jnp.full((1,), NGRID - 1, jnp.int32), middle])
    return jax.random.permutation(order_key, chosen).astype(jnp.int32)


def with_ends(entries, stream_key, smallest, top_value):
    index_at = [jax.random.randint(jax.random.fold_in(stream_key, axis), (), 0, length) for axis, length in enumerate(entries.shape)]
    widest = entries.shape.index(max(entries.shape))
    beside = index_at[:widest] + [(index_at[widest] + 1) % entries.shape[widest]] + index_at[widest + 1:]
    return entries.at[tuple(index_at)].set(smallest).at[tuple(beside)].set(top_value)


def block_scale(stream_key, dims, cuts, least, high):
    loudness, own = 1.0, jax.random.fold_in(stream_key, 6)
    for position, parts in cuts:
        draws = jnp.exp(jax.random.uniform(jax.random.fold_in(own, position), (parts,), jnp.float32, least / len(cuts), high / len(cuts)))
        loudness = loudness * jnp.repeat(draws, dims[position] // parts).reshape([-1 if axis == position else 1 for axis in range(len(dims))])
    return loudness


def gaussian(rng, shape, deviation, bound, shards=(), kind=jnp.bfloat16):
    result = jax.random.normal(rng, shape, jnp.float32) * deviation
    if len(shards) > 0:
        result = block_scale(rng, shape, shards, -0.22, 0.18) * result
    return jnp.clip(result, min=-bound, max=bound).astype(kind)


def setup_inputs(seed: int = 0) -> dict:
    splits = jax.random.split(jax.random.key(seed), 10)
    occ_orbitals = gaussian(splits[0], (NP, NOCC), NOCC ** -0.5, 0.1875, ((0, 32),))
    virt_orbitals = gaussian(splits[1], (NP, NVIR), NVIR ** -0.5, 0.1875, ((0, 32),))
    columns = gaussian(splits[2], (NP, NCOL), 1.0, 6.0, ((0, 32),))
    occ_energies = jnp.clip(jax.random.uniform(splits[3], (NOCC,), jnp.float32, -3.0, -0.1), -3.0, -0.1)
    vir_energies = jnp.clip(jax.random.uniform(splits[4], (NVIR,), jnp.float32, 0.1, 3.0), 0.1, 3.0)
    tau_index = draw_tau_index(jax.random.fold_in(splits[9], 71), 0)
    quad_weights = jnp.clip(jnp.exp(jax.random.uniform(splits[6], (NTAU,), jnp.float32, math.log(0.05), math.log(0.5))), 0.05, 0.5)
    frequencies = jnp.clip(jnp.exp(jax.random.uniform(splits[7], (NFREQ,), jnp.float32, math.log(0.2), math.log(2.0))), 0.2, 2.0)
    distance_kept = with_ends((jax.random.randint(splits[8], (N_PTS,), 0, 4) < 3).astype(jnp.int32), jax.random.fold_in(splits[8], 1), 0, 1)
    return {"occ_orbitals": occ_orbitals, "virt_orbitals": virt_orbitals, "columns": columns, "occ_energies": occ_energies, "vir_energies": vir_energies, "tau_index": tau_index, "quad_weights": quad_weights, "frequencies": frequencies, "distance_kept": distance_kept}


def reference(occ_orbitals, virt_orbitals, columns, occ_energies, vir_energies, tau_index, quad_weights, frequencies, distance_kept):
    highest = lax.Precision.HIGHEST
    times = 0.05 * jnp.exp(tau_index.astype(jnp.float32) * jnp.float32(math.log(1.5)))
    cosine = -quad_weights[None, :] * jnp.cos(frequencies[:, None] * times[None, :])
    occ_full = occ_orbitals.astype(jnp.float32)
    vir_full = virt_orbitals.astype(jnp.float32)
    col_full = columns.astype(jnp.float32)
    occ_blocks = occ_full.reshape(N_PTS, BP, NOCC)
    vir_blocks = vir_full.reshape(N_PTS, BP, NVIR)
    col_block = jnp.arange(N_PTS * BP, dtype=jnp.int32) // BP
    occ_decay = jnp.exp(occ_energies[None, :] * times[:, None])
    vir_decay = jnp.exp(-vir_energies[None, :] * times[:, None])

    def one_block(carry, inputs):
        row_block, occ_rows, vir_rows = inputs
        occ_scaled = (occ_rows[None] * occ_decay[:, None, :]).astype(jnp.bfloat16).astype(jnp.float32)
        vir_scaled = (vir_rows[None] * vir_decay[:, None, :]).astype(jnp.bfloat16).astype(jnp.float32)
        green_occ = jnp.dot(occ_scaled.reshape(NTAU * BP, NOCC), occ_full.T, precision=highest, preferred_element_type=jnp.float32)
        green_vir = jnp.dot(vir_scaled.reshape(NTAU * BP, NVIR), vir_full.T, precision=highest, preferred_element_type=jnp.float32)
        product = (green_occ * green_vir).reshape(NTAU, BP, N_PTS * BP)
        chi = jnp.einsum("wk,krs->wrs", cosine, product, precision=highest)
        distance = (col_block - row_block) % N_PTS
        kept = distance_kept[distance].astype(jnp.float32)
        chi = chi * kept[None, None, :]
        answer = jnp.einsum("wrs,sc->wcr", chi, col_full, precision=highest)
        return carry, answer

    _, pieces = lax.scan(one_block, jnp.int32(0), (jnp.arange(N_PTS, dtype=jnp.int32), occ_blocks, vir_blocks))
    return jnp.transpose(pieces, (1, 2, 0, 3)).reshape(NFREQ, NCOL, N_PTS * BP)
```

```python
import functools
import math

import jax
import jax.numpy as jnp
from jax import lax
from jax.experimental import pallas as pl
from jax.experimental.pallas import tpu as pltpu
from jax.sharding import PartitionSpec as P


AXES = ("pts", "grp")
NZ, NYL, NC, NYH, NX = 8, 2, 2, 2, 4
PLANES = (0, 4, 2, -2, 1, -1, 3, -3)
TILE = 64


def coords(p, g):
    return p // (NYL * NC), p // NC % NYL, p % NC, g // NX, g % NX


def pairs(to):
    out = []
    for p in range(NZ * NYL * NC):
        for g in range(NYH * NX):
            z, yl, c, yh, x = to(*coords(p, g))
            q = (z % NZ * NYL + yl % NYL) * NC + c % NC
            out.append((p * NYH * NX + g, q * NYH * NX + yh % NYH * NX + x % NX))
    return out


def move_y(z, yl, c, yh, x, by):
    y = (yh * NYL + yl + by) % (NYH * NYL)
    return z, y % NYL, c, y // NYL, x


def send(array, to):
    return lax.ppermute(array, AXES, pairs(to))


def fetch(array, k):
    def to(z, yl, c, yh, x):
        goal = (x - k) % NX
        return z - PLANES[yh * NX + goal], yl, c, yh, goal

    return send(array, to)


def from_core(array):
    return send(array, lambda z, yl, c, yh, x: (z, yl, c + 1, yh, x))


def from_y(array, by):
    return send(array, lambda *at: move_y(*at, -by))


def chunk_kernel(sizes, taus, states, last, cos_ref, kept_ref, occ_ref, vir_ref, *refs):
    n = len(sizes)
    pieces, rest = refs[:n], refs[n:]
    if last:
        acc_ref, out_ref, s_occ, s_vir, s_col = rest
    else:
        acc_ref = rest[0] if len(rest) == 5 else None
        out_ref, s_occ, s_vir, s_col = rest[-4:]
    at = 0
    for i, size in enumerate(sizes):
        rows = pl.ds(at, size)
        s_occ[rows, :] = pieces[i][:, :states]
        s_vir[rows, :] = pieces[i][:, states : 2 * states]
        kept = kept_ref[i].astype(jnp.bfloat16)
        s_col[rows, :] = pieces[i][:, 2 * states :] * kept
        at += size
    contract = (((1,), (1,)), ((), ()))
    tile = 2 * TILE if last else TILE
    count = occ_ref.shape[1] // tile

    def step(i):
        rows = pl.ds(pl.multiple_of(i * tile, tile), tile)
        left = occ_ref[:, rows, :].reshape(taus * tile, states)
        g_occ = lax.dot_general(left, s_occ[...], contract, preferred_element_type=jnp.float32)
        left = vir_ref[:, rows, :].reshape(taus * tile, states)
        g_vir = lax.dot_general(left, s_vir[...], contract, preferred_element_type=jnp.float32)
        product = (g_occ * g_vir).reshape(taus, tile, at)
        for w in range(2):
            chi = cos_ref[w * taus] * product[0]
            for k in range(1, taus):
                chi = chi + cos_ref[w * taus + k] * product[k]
            high = chi.astype(jnp.bfloat16)
            low = (chi - high.astype(jnp.float32)).astype(jnp.bfloat16)
            answer = jnp.dot(high, s_col[...], preferred_element_type=jnp.float32)
            answer = answer + jnp.dot(low, s_col[...], preferred_element_type=jnp.float32)
            if acc_ref is not None:
                answer = answer + acc_ref[w, rows, :]
            if last:
                groups, _, width, _ = out_ref.shape
                turned = answer.T.astype(jnp.bfloat16)
                out_ref[:, w, :, rows] = turned.reshape(groups, width, tile)
            else:
                out_ref[w, rows, :] = answer

    if last:
        for i in range(count):
            step(i)
    else:
        pl.loop(0, count)(step)


def chunk_term(cosine, kept, occ_scaled, vir_scaled, pieces, total, last):
    taus, points, states = occ_scaled.shape
    columns = pieces[0].shape[1] - 2 * states
    sizes = tuple(piece.shape[0] for piece in pieces)
    width = sum(sizes)
    if last:
        out = jax.ShapeDtypeStruct((8, 2, columns // 8, points), jnp.bfloat16)
    else:
        out = jax.ShapeDtypeStruct((2, points, columns), jnp.float32)
    carried = () if total is None else (total,)
    vmem = pl.BlockSpec(memory_space=pltpu.VMEM)
    smem = pl.BlockSpec(memory_space=pltpu.SMEM)
    return pl.pallas_call(
        functools.partial(chunk_kernel, sizes, taus, states, last),
        out_shape=out,
        in_specs=[smem, smem] + [vmem] * (2 + len(pieces) + len(carried)),
        out_specs=vmem,
        scratch_shapes=[
            pltpu.VMEM((width, states), jnp.bfloat16),
            pltpu.VMEM((width, states), jnp.bfloat16),
            pltpu.VMEM((width, columns), jnp.bfloat16),
        ],
        compiler_params=pltpu.CompilerParams(vmem_limit_bytes=40 * 1024 * 1024),
        cost_estimate=pl.CostEstimate(
            flops=4 * taus * points * states * width,
            bytes_accessed=10 * 1024 * 1024,
            transcendentals=0,
        ),
    )(cosine, kept, occ_scaled, vir_scaled, *pieces, *carried)


def per_device(
    occ_orbitals,
    virt_orbitals,
    columns,
    occ_energies,
    vir_energies,
    tau_index,
    quad_weights,
    frequencies,
    distance_kept,
):
    points = occ_orbitals.shape[0]
    rows = points // NX
    parts = [
        jnp.concatenate([a[k * rows : (k + 1) * rows] for a in (occ_orbitals, virt_orbitals, columns)], axis=1)
        for k in range(NX)
    ]
    arrived = [fetch(parts[k], k) for k in range(NX)]

    times = 0.05 * jnp.exp(tau_index.astype(jnp.float32) * jnp.float32(math.log(1.5)))
    cosine = (-quad_weights[None, :] * jnp.cos(frequencies[:, None] * times[None, :])).reshape(-1)
    occ_decay = jnp.exp(occ_energies[None, :] * times[:, None])
    vir_decay = jnp.exp(-vir_energies[None, :] * times[:, None])
    occ_scaled = (occ_orbitals[None].astype(jnp.float32) * occ_decay[:, None, :]).astype(jnp.bfloat16)
    vir_scaled = (virt_orbitals[None].astype(jnp.float32) * vir_decay[:, None, :]).astype(jnp.bfloat16)

    me = lax.axis_index("pts")
    group = lax.axis_index("grp")
    z, yl, c = me // (NYL * NC), me // NC % NYL, me % NC
    yh, x = group // NX, group % NX
    planes = jnp.array(PLANES, jnp.int32)

    def kept_of(other_yl, other_yh, other_c):
        plane = (z + planes[other_yh * NX + x]) % NZ
        block = (plane * NYL + other_yl) * NC + other_c
        return distance_kept[(block - me) % (NZ * NYL * NC)]

    def kept_y(by):
        _, other_yl, _, other_yh, _ = move_y(z, yl, c, yh, x, by)
        return [kept_of(other_yl, other_yh, c), kept_of(other_yl, other_yh, 1 - c)]

    own = [kept_of(yl, yh, c), kept_of(yl, yh, 1 - c)]
    up, down = kept_y(1), kept_y(-1)

    total = None
    for k in range(NX):
        part = arrived[k]
        last = k == NX - 1
        if last:
            half = rows // 2
            near = [from_y(part[:half], 1), from_y(part[half:], -1)]
            marks = own + up + down
        else:
            by = 1 if k % 2 == 0 else -1
            near = [from_y(part, by)]
            marks = own + (up if by == 1 else down)
        pieces = [part, from_core(part)]
        for piece in near:
            pieces += [piece, from_core(piece)]
        kept = jnp.stack(marks).astype(jnp.float32)
        total = chunk_term(cosine, kept, occ_scaled, vir_scaled, pieces, total, last)

    spread = lax.all_to_all(total, "grp", split_axis=0, concat_axis=0, tiled=True)
    return spread.astype(jnp.float32).sum(axis=0)


def solution(mesh):
    placed = (P("pts", None), P("pts", None), P("pts", None), P(), P(), P(), P(), P(), P())
    return jax.shard_map(
        per_device, mesh=mesh, in_specs=placed, out_specs=P(None, "grp", "pts"), check_vma=False
    )
```

```python
import functools
import math

import jax
import jax.numpy as jnp
from jax import lax
from jax.experimental import pallas as pl
from jax.experimental.pallas import tpu as pltpu
from jax.sharding import PartitionSpec as P


AXES = ("pts", "grp")
NZ, NYL, NC, NYH, NX = 8, 2, 2, 2, 4
PLANES = (
    (0, 5, 6, 3, 4, 1, 2, 7),
    (1, 3, 7, 5, 2, 0, 4, 6),
    (2, 6, 4, 1, 7, 3, 5, 0),
    (3, 7, 1, 4, 6, 2, 0, 5),
    (4, 1, 2, 7, 0, 5, 6, 3),
    (5, 0, 3, 6, 1, 4, 7, 2),
    (6, 4, 0, 2, 5, 7, 3, 1),
    (7, 2, 5, 0, 3, 6, 1, 4),
)
TILE = 128
CHUNKS = (64, 64, 64, 64)


def coords(p, g):
    return p // (NYL * NC), p // NC % NYL, p % NC, g // NX, g % NX


def place(z, yl, c, yh, x):
    return (z % NZ * NYL + yl % NYL) * NC + c % NC, yh % NYH * NX + x % NX


def take(array, source):
    found = []
    for p in range(NZ * NYL * NC):
        for g in range(NYH * NX):
            q, h = place(*source(*coords(p, g)))
            found.append((q * NYH * NX + h, p * NYH * NX + g))
    return lax.ppermute(array, AXES, found)


def move_y(z, yl, c, yh, x, by):
    y = (yh * NYL + yl + by) % (NYH * NYL)
    return z, y % NYL, c, y // NYL, x


def from_plane(array):
    return take(array, lambda z, yl, c, yh, x: (PLANES[yh * NX + x][z], yl, c, yh, x))


def from_core(array):
    return take(array, lambda z, yl, c, yh, x: (z, yl, c + 1, yh, x))


def from_y(array, by):
    return take(array, lambda *at: move_y(*at, by))


def scale_kernel(occ_ref, vir_ref, occ_decay_ref, vir_decay_ref, occ_out, vir_out):
    step = 16

    def body(i):
        rows = pl.ds(pl.multiple_of(i * step, step), step)
        for source, decay, out in ((occ_ref, occ_decay_ref, occ_out), (vir_ref, vir_decay_ref, vir_out)):
            values = source[rows, :].astype(jnp.float32)
            for k in range(out.shape[0]):
                out[k, rows, :] = (values * decay[k : k + 1, :]).astype(jnp.bfloat16)

    pl.loop(0, occ_ref.shape[0] // step)(body)


def scaled(occ, vir, occ_decay, vir_decay):
    shape = jax.ShapeDtypeStruct((occ_decay.shape[0], *occ.shape), jnp.bfloat16)
    vmem = pl.BlockSpec(memory_space=pltpu.VMEM)
    return pl.pallas_call(
        scale_kernel,
        out_shape=(shape, shape),
        in_specs=[vmem] * 4,
        out_specs=(vmem, vmem),
        compiler_params=pltpu.CompilerParams(vmem_limit_bytes=16 * 1024 * 1024),
        cost_estimate=pl.CostEstimate(flops=10**8, bytes_accessed=10**7, transcendentals=0),
    )(occ, vir, occ_decay, vir_decay)


def chunk_kernel(segments, n, last, cos_ref, kept_ref, planes_ref, occ_ref, vir_ref, *refs):
    pieces, rest = refs[:n], refs[n:]
    acc_ref = None if len(rest) == 5 else rest[0]
    out_ref, s_occ, s_vir, s_col, parts = rest[-5:]
    taus, points, states = occ_ref.shape
    me = lax.axis_index("pts")
    z, yl, c, yh, x = coords(me, lax.axis_index("grp"))
    at = 0
    for i, first, size, by, other in segments:
        _, s_yl, _, s_yh, _ = move_y(z, yl, c, yh, x, by)
        s_c = 1 - c if other else c
        plane = planes_ref[(s_yh * NX + x) * NZ + z]
        block = (plane * NYL + s_yl) * NC + s_c
        count = kept_ref.shape[0]
        kept = kept_ref[(block - me + count) % count].astype(jnp.float32).astype(jnp.bfloat16)
        here, there = pl.ds(at, size), pl.ds(first, size)
        s_occ[here, :] = pieces[i][there, :states]
        s_vir[here, :] = pieces[i][there, states : 2 * states]
        s_col[here, :] = pieces[i][there, 2 * states :] * kept
        at += size
    contract = (((1,), (1,)), ((), ()))

    def step(i):
        rows = pl.ds(pl.multiple_of(i * TILE, TILE), TILE)
        left = occ_ref[:, rows, :].reshape(taus * TILE, states)
        g_occ = lax.dot_general(left, s_occ[...], contract, preferred_element_type=jnp.float32)
        left = vir_ref[:, rows, :].reshape(taus * TILE, states)
        g_vir = lax.dot_general(left, s_vir[...], contract, preferred_element_type=jnp.float32)
        product = (g_occ * g_vir).reshape(taus, TILE, at)
        for w in range(2):
            chi = cos_ref[w * taus] * product[0]
            for k in range(1, taus):
                chi = chi + cos_ref[w * taus + k] * product[k]
            high = chi.astype(jnp.bfloat16)
            parts[w, 0, rows, :] = high
            parts[w, 1, rows, :] = (chi - high.astype(jnp.float32)).astype(jnp.bfloat16)

    pl.loop(0, points // TILE)(step)
    answers = jnp.dot(parts[...].reshape(4 * points, at), s_col[...], preferred_element_type=jnp.float32)
    answers = answers.reshape(2, 2, points, s_col.shape[1])
    for w in range(2):
        answer = answers[w, 0] + answers[w, 1]
        if acc_ref is not None:
            answer = answer + acc_ref[w]
        if last:
            groups, _, width, _ = out_ref.shape
            out_ref[:, w] = answer.T.astype(jnp.bfloat16).reshape(groups, width, points)
        else:
            out_ref[w] = answer


def chunk_term(cosine, kept, planes, occ_scaled, vir_scaled, pieces, segments, total, last):
    taus, points, states = occ_scaled.shape
    columns = pieces[0].shape[1] - 2 * states
    width = sum(segment[2] for segment in segments)
    if last:
        out = jax.ShapeDtypeStruct((NYH * NX, 2, columns // (NYH * NX), points), jnp.bfloat16)
    else:
        out = jax.ShapeDtypeStruct((2, points, columns), jnp.float32)
    carried = () if total is None else (total,)
    vmem = pl.BlockSpec(memory_space=pltpu.VMEM)
    smem = pl.BlockSpec(memory_space=pltpu.SMEM)
    return pl.pallas_call(
        functools.partial(chunk_kernel, segments, len(pieces), last),
        out_shape=out,
        in_specs=[smem] * 3 + [vmem] * (2 + len(pieces) + len(carried)),
        out_specs=vmem,
        scratch_shapes=[
            pltpu.VMEM((width, states), jnp.bfloat16),
            pltpu.VMEM((width, states), jnp.bfloat16),
            pltpu.VMEM((width, columns), jnp.bfloat16),
            pltpu.VMEM((2, 2, points, width), jnp.bfloat16),
        ],
        compiler_params=pltpu.CompilerParams(vmem_limit_bytes=20 * 1024 * 1024),
        cost_estimate=pl.CostEstimate(
            flops=4 * taus * points * states * width, bytes_accessed=10**7, transcendentals=0
        ),
    )(cosine, kept, planes, occ_scaled, vir_scaled, *pieces, *carried)


def per_device(
    occ_orbitals,
    virt_orbitals,
    columns,
    occ_energies,
    vir_energies,
    tau_index,
    quad_weights,
    frequencies,
    distance_kept,
):
    count = len(CHUNKS)
    arrived, at = [], 0
    for size in CHUNKS:
        part = [a[at : at + size] for a in (occ_orbitals, virt_orbitals, columns)]
        at += size
        arrived.append(from_plane(jnp.concatenate(part, axis=1)))

    times = 0.05 * jnp.exp(tau_index.astype(jnp.float32) * jnp.float32(math.log(1.5)))
    cosine = (-quad_weights[None, :] * jnp.cos(frequencies[:, None] * times[None, :])).reshape(-1)
    occ_decay = jnp.exp(occ_energies[None, :] * times[:, None])
    vir_decay = jnp.exp(-vir_energies[None, :] * times[:, None])
    occ_scaled, vir_scaled = scaled(occ_orbitals, virt_orbitals, occ_decay, vir_decay)
    planes = jnp.array(PLANES, jnp.int32).reshape(-1)

    total = None
    for k, part in enumerate(arrived):
        size = CHUNKS[k]
        last = k == count - 1
        if last:
            half = size // 2
            near = [from_y(part[:half], 1), from_y(part[half:], -1)]
            ways = [(half, 1), (half, -1)]
        else:
            near = [from_y(part, 1 if k % 2 == 0 else -1)]
            ways = [(size, 1 if k % 2 == 0 else -1)]
        beside = from_core(jnp.concatenate([part, *near]))
        pieces = [part, *near, beside]
        segments = [(0, 0, size, 0, False)]
        for i, (rows, by) in enumerate(ways):
            segments.append((1 + i, 0, rows, by, False))
        segments.append((len(pieces) - 1, 0, size, 0, True))
        at = size
        for rows, by in ways:
            segments.append((len(pieces) - 1, at, rows, by, True))
            at += rows
        total = chunk_term(
            cosine, distance_kept, planes, occ_scaled, vir_scaled, pieces, tuple(segments), total, last
        )

    spread = lax.all_to_all(total, "grp", split_axis=0, concat_axis=0, tiled=True)
    return spread.astype(jnp.float32).sum(axis=0)


def solution(mesh):
    placed = (P("pts", None), P("pts", None), P("pts", None), P(), P(), P(), P(), P(), P())
    return jax.shard_map(
        per_device, mesh=mesh, in_specs=placed, out_specs=P(None, "grp", "pts"), check_vma=False
    )
```

```python
import functools
import math

import jax
import jax.numpy as jnp
from jax import lax
from jax.experimental import pallas as pl
from jax.experimental.pallas import tpu as pltpu
from jax.sharding import PartitionSpec as P


AXES = ("pts", "grp")
NZ, NYL, NC, NYH, NX = 8, 2, 2, 2, 4
PLANES = (
    (0, 5, 6, 3, 4, 1, 2, 7),
    (1, 3, 7, 5, 2, 0, 4, 6),
    (2, 6, 4, 1, 7, 3, 5, 0),
    (3, 7, 1, 4, 6, 2, 0, 5),
    (4, 1, 2, 7, 0, 5, 6, 3),
    (5, 0, 3, 6, 1, 4, 7, 2),
    (6, 4, 0, 2, 5, 7, 3, 1),
    (7, 2, 5, 0, 3, 6, 1, 4),
)
TILE = 128
CHUNKS = (128, 64, 64)


def coords(p, g):
    return p // (NYL * NC), p // NC % NYL, p % NC, g // NX, g % NX


def place(z, yl, c, yh, x):
    return (z % NZ * NYL + yl % NYL) * NC + c % NC, yh % NYH * NX + x % NX


def take(array, source):
    found = []
    for p in range(NZ * NYL * NC):
        for g in range(NYH * NX):
            q, h = place(*source(*coords(p, g)))
            found.append((q * NYH * NX + h, p * NYH * NX + g))
    return lax.ppermute(array, AXES, found)


def move_y(z, yl, c, yh, x, by):
    y = (yh * NYL + yl + by) % (NYH * NYL)
    return z, y % NYL, c, y // NYL, x


def from_plane(array):
    return take(array, lambda z, yl, c, yh, x: (PLANES[yh * NX + x][z], yl, c, yh, x))


def from_core(array):
    return take(array, lambda z, yl, c, yh, x: (z, yl, c + 1, yh, x))


def from_y(array, by):
    return take(array, lambda *at: move_y(*at, by))


def pack_kernel(occ_ref, vir_ref, col_ref, *refs):
    outs, sems = refs[:-1], refs[-1]
    copies, at = [], 0
    for out in outs:
        size, left = out.shape[0], 0
        for source in (occ_ref, vir_ref, col_ref):
            width = source.shape[1]
            copies.append(
                pltpu.make_async_copy(
                    source.at[pl.ds(at, size), :], out.at[:, pl.ds(left, width)], sems.at[len(copies)]
                )
            )
            left += width
        at += size
    for copy in copies:
        copy.start()
    for copy in copies:
        copy.wait()


def packed(occ, vir, col):
    width = occ.shape[1] + vir.shape[1] + col.shape[1]
    vmem = pl.BlockSpec(memory_space=pltpu.VMEM)
    return pl.pallas_call(
        pack_kernel,
        out_shape=[jax.ShapeDtypeStruct((size, width), jnp.bfloat16) for size in CHUNKS],
        in_specs=[pl.BlockSpec(memory_space=pltpu.HBM)] * 3,
        out_specs=[vmem] * len(CHUNKS),
        scratch_shapes=[pltpu.SemaphoreType.DMA((3 * len(CHUNKS),))],
        compiler_params=pltpu.CompilerParams(vmem_limit_bytes=65000000),
        cost_estimate=pl.CostEstimate(flops=10**6, bytes_accessed=3 * 10**6, transcendentals=0),
    )(occ, vir, col)


def join_kernel(*refs):
    *pieces, out = refs
    at = 0
    for piece in pieces:
        out[pl.ds(at, piece.shape[0]), :] = piece[...]
        at += piece.shape[0]


def split_kernel(piece, *outs):
    at = 0
    for out in outs:
        out[...] = piece[pl.ds(at, out.shape[0]), :]
        at += out.shape[0]


def moved(kernel, pieces, sizes):
    vmem = pl.BlockSpec(memory_space=pltpu.VMEM)
    return pl.pallas_call(
        kernel,
        out_shape=[jax.ShapeDtypeStruct((size, pieces[0].shape[1]), pieces[0].dtype) for size in sizes],
        in_specs=[vmem] * len(pieces),
        out_specs=[vmem] * len(sizes),
        compiler_params=pltpu.CompilerParams(vmem_limit_bytes=8 * 1024 * 1024),
        cost_estimate=pl.CostEstimate(flops=10**6, bytes_accessed=10**6, transcendentals=0),
    )(*pieces)


def scale_kernel(
    sources, cos_ref, kept_ref, planes_ref, occ_ref, vir_ref, occ_decay_ref, vir_decay_ref,
    occ_out, vir_out, cos_out, kept_out,
):
    me = lax.axis_index("pts")
    z, yl, c, yh, x = coords(me, lax.axis_index("grp"))
    count = kept_ref.shape[0]
    for i, (by, other) in enumerate(sources):
        _, s_yl, _, s_yh, _ = move_y(z, yl, c, yh, x, by)
        s_c = 1 - c if other else c
        plane = planes_ref[(s_yh * NX + x) * NZ + z]
        block = (plane * NYL + s_yl) * NC + s_c
        kept = kept_ref[(block - me + count) % count].astype(jnp.float32)
        kept_out[i : i + 1, :] = jnp.full((1, kept_out.shape[1]), kept, jnp.float32)
    for i in range(cos_out.shape[0]):
        cos_out[i : i + 1, :] = jnp.full((1, cos_out.shape[1]), cos_ref[i], jnp.float32)
    step = 16

    def body(i):
        rows = pl.ds(pl.multiple_of(i * step, step), step)
        for source, decay, out in ((occ_ref, occ_decay_ref, occ_out), (vir_ref, vir_decay_ref, vir_out)):
            values = source[rows, :].astype(jnp.float32)
            for k in range(out.shape[0]):
                out[k, rows, :] = (values * decay[k : k + 1, :]).astype(jnp.bfloat16)

    pl.loop(0, occ_ref.shape[0] // step)(body)


SOURCES = ((0, False), (0, True), (1, False), (1, True), (-1, False), (-1, True))


def scaled(cosine, kept, planes, occ, vir, occ_decay, vir_decay, columns):
    shape = jax.ShapeDtypeStruct((occ_decay.shape[0], *occ.shape), jnp.bfloat16)
    rows = jax.ShapeDtypeStruct((cosine.shape[0], 256), jnp.float32)
    marks = jax.ShapeDtypeStruct((8, columns), jnp.float32)
    vmem = pl.BlockSpec(memory_space=pltpu.VMEM)
    smem = pl.BlockSpec(memory_space=pltpu.SMEM)
    return pl.pallas_call(
        functools.partial(scale_kernel, SOURCES),
        out_shape=(shape, shape, rows, marks),
        in_specs=[smem] * 3 + [vmem] * 4,
        out_specs=(vmem,) * 4,
        compiler_params=pltpu.CompilerParams(vmem_limit_bytes=16 * 1024 * 1024),
        cost_estimate=pl.CostEstimate(flops=10**8, bytes_accessed=10**7, transcendentals=0),
    )(cosine, kept, planes, occ, vir, occ_decay, vir_decay)


def chunk_kernel(segments, n, last, cos_ref, kept_ref, occ_ref, vir_ref, *refs):
    pieces, rest = refs[:n], refs[n:]
    acc_ref = None if len(rest) == 5 else rest[0]
    out_ref, s_occ, s_vir, s_col, parts = rest[-5:]
    taus, points, states = occ_ref.shape
    at = 0
    for i, first, size, kind in segments:
        here, there = pl.ds(at, size), pl.ds(first, size)
        s_occ[here, :] = pieces[i][there, :states]
        s_vir[here, :] = pieces[i][there, states : 2 * states]
        s_col[here, :] = pieces[i][there, 2 * states :] * kept_ref[kind : kind + 1, :].astype(jnp.bfloat16)
        at += size
    contract = (((1,), (1,)), ((), ()))

    def step(i):
        rows = pl.ds(pl.multiple_of(i * TILE, TILE), TILE)
        left = occ_ref[:, rows, :].reshape(taus * TILE, states)
        g_occ = lax.dot_general(left, s_occ[...], contract, preferred_element_type=jnp.float32)
        left = vir_ref[:, rows, :].reshape(taus * TILE, states)
        g_vir = lax.dot_general(left, s_vir[...], contract, preferred_element_type=jnp.float32)
        product = (g_occ * g_vir).reshape(taus, TILE, at)
        for w in range(2):
            chi = cos_ref[w * taus : w * taus + 1, :] * product[0]
            for k in range(1, taus):
                chi = chi + cos_ref[w * taus + k : w * taus + k + 1, :] * product[k]
            high = chi.astype(jnp.bfloat16)
            parts[w, 0, rows, :] = high
            parts[w, 1, rows, :] = (chi - high.astype(jnp.float32)).astype(jnp.bfloat16)

    pl.loop(0, points // TILE)(step)
    answers = jnp.dot(parts[...].reshape(4 * points, at), s_col[...], preferred_element_type=jnp.float32)
    answers = answers.reshape(2, 2, points, s_col.shape[1])
    for w in range(2):
        answer = answers[w, 0] + answers[w, 1]
        if acc_ref is not None:
            answer = answer + acc_ref[w]
        if last:
            groups, _, width, _ = out_ref.shape
            out_ref[:, w] = answer.T.astype(jnp.bfloat16).reshape(groups, width, points)
        else:
            out_ref[w] = answer


def chunk_term(cosine, kept, occ_scaled, vir_scaled, pieces, segments, total, last):
    taus, points, states = occ_scaled.shape
    columns = pieces[0].shape[1] - 2 * states
    width = sum(segment[2] for segment in segments)
    if last:
        out = jax.ShapeDtypeStruct((NYH * NX, 2, columns // (NYH * NX), points), jnp.bfloat16)
    else:
        out = jax.ShapeDtypeStruct((2, points, columns), jnp.float32)
    carried = () if total is None else (total,)
    vmem = pl.BlockSpec(memory_space=pltpu.VMEM)
    return pl.pallas_call(
        functools.partial(chunk_kernel, segments, len(pieces), last),
        out_shape=out,
        in_specs=[vmem] * (4 + len(pieces) + len(carried)),
        out_specs=vmem,
        scratch_shapes=[
            pltpu.VMEM((width, states), jnp.bfloat16),
            pltpu.VMEM((width, states), jnp.bfloat16),
            pltpu.VMEM((width, columns), jnp.bfloat16),
            pltpu.VMEM((2, 2, points, width), jnp.bfloat16),
        ],
        compiler_params=pltpu.CompilerParams(vmem_limit_bytes=20 * 1024 * 1024),
        cost_estimate=pl.CostEstimate(
            flops=4 * taus * points * states * width, bytes_accessed=10**7, transcendentals=0
        ),
    )(cosine, kept, occ_scaled, vir_scaled, *pieces, *carried)


def per_device(
    occ_orbitals,
    virt_orbitals,
    columns,
    occ_energies,
    vir_energies,
    tau_index,
    quad_weights,
    frequencies,
    distance_kept,
):
    parts = packed(occ_orbitals, virt_orbitals, columns)
    arrived = []
    for part in parts:
        arrived.append(from_plane(part))

    times = 0.05 * jnp.exp(tau_index.astype(jnp.float32) * jnp.float32(math.log(1.5)))
    cosine = (-quad_weights[None, :] * jnp.cos(frequencies[:, None] * times[None, :])).reshape(-1)
    occ_decay = jnp.exp(occ_energies[None, :] * times[:, None])
    vir_decay = jnp.exp(-vir_energies[None, :] * times[:, None])
    planes = jnp.array(PLANES, jnp.int32).reshape(-1)
    occ_scaled, vir_scaled, cos_rows, marks = scaled(
        cosine, distance_kept, planes, occ_orbitals, virt_orbitals, occ_decay, vir_decay, columns.shape[1]
    )

    def exchanged(k, sizes, steps):
        part = arrived[k]
        halves = moved(split_kernel, [part], sizes) if len(sizes) > 1 else [part]
        near = [from_y(half, by) for half, by in zip(halves, steps)]
        (joined,) = moved(join_kernel, [part, *near], [part.shape[0] + sum(sizes)])
        beside = from_core(joined)
        return [part, *near, beside]

    a = exchanged(0, (64, 64), (1, -1))
    b = exchanged(1, (64,), (1,))
    c = exchanged(2, (32, 32), (1, -1))
    work = (
        ((a[0], a[1], a[3]), ((0, 0, 64, 0), (1, 0, 64, 2), (2, 0, 64, 1), (2, 128, 64, 3))),
        ((a[0], a[2], a[3]), ((0, 64, 64, 0), (1, 0, 64, 4), (2, 64, 64, 1), (2, 192, 64, 5))),
        ((b[0], b[1], b[2]), ((0, 0, 64, 0), (1, 0, 64, 2), (2, 0, 64, 1), (2, 64, 64, 3))),
        (
            (c[0], c[1], c[2], c[3]),
            ((0, 0, 64, 0), (1, 0, 32, 2), (2, 0, 32, 4), (3, 0, 64, 1), (3, 64, 32, 3), (3, 96, 32, 5)),
        ),
    )
    total = None
    for k, (pieces, segments) in enumerate(work):
        total = chunk_term(
            cos_rows, marks, occ_scaled, vir_scaled, pieces, segments, total, k == len(work) - 1
        )

    spread = lax.all_to_all(total, "grp", split_axis=0, concat_axis=0, tiled=True)
    return spread.astype(jnp.float32).sum(axis=0)


def solution(mesh):
    placed = (P("pts", None), P("pts", None), P("pts", None), P(), P(), P(), P(), P(), P())
    return jax.shard_map(per_device, mesh=mesh, in_specs=placed, out_specs=P(None, "grp", "pts"), check_vma=False)
```

```python
import math

import jax
import jax.numpy as jnp
from jax import lax
from jax.experimental import pallas as pl
from jax.experimental.pallas import tpu as pltpu
from jax.sharding import Mesh, PartitionSpec as P


AXES = ("z", "yl", "c", "yh", "x")
SIZES = (8, 2, 2, 2, 4)
NZ, NYL, NC, NYH, NX = SIZES
PLANES = (
    (0, 5, 6, 3, 4, 1, 2, 7),
    (1, 3, 7, 5, 2, 0, 4, 6),
    (2, 6, 4, 1, 7, 3, 5, 0),
    (3, 7, 1, 4, 6, 2, 0, 5),
    (4, 1, 2, 7, 0, 5, 6, 3),
    (5, 0, 3, 6, 1, 4, 7, 2),
    (6, 4, 0, 2, 5, 7, 3, 1),
    (7, 2, 5, 0, 3, 6, 1, 4),
)
TILE = 128
VMEM = pl.BlockSpec(memory_space=pltpu.VMEM)
SMEM = pl.BlockSpec(memory_space=pltpu.SMEM)
MIB = 1024 * 1024


def place(at):
    index = 0
    for value, size in zip(at, SIZES):
        index = index * size + value % size
    return index


def everywhere(at=()):
    if len(at) == len(SIZES):
        return [at]
    return [full for i in range(SIZES[len(at)]) for full in everywhere((*at, i))]


def take(array, source):
    return lax.ppermute(array, AXES, [(place(source(*at)), place(at)) for at in everywhere()])


def from_plane(array):
    return take(array, lambda z, yl, c, yh, x: (PLANES[yh * NX + x][z], yl, c, yh, x))


def from_core(array):
    return take(array, lambda z, yl, c, yh, x: (z, yl, c + 1, yh, x))


def from_y(array, by):
    def source(z, yl, c, yh, x):
        y = (yh * NYL + yl + by) % (NYH * NYL)
        return z, y % NYL, c, y // NYL, x

    return take(array, source)


def cost(flops):
    return pl.CostEstimate(flops=int(flops), bytes_accessed=4 * MIB, transcendentals=0)


def scale_rows(source, decay, out):
    step = 16

    def body(i):
        rows = pl.ds(pl.multiple_of(i * step, step), step)
        values = source[rows, :].astype(jnp.float32)
        for k in range(out.shape[0]):
            out[k, rows, :] = (values * decay[k : k + 1, :]).astype(jnp.bfloat16)

    pl.loop(0, source.shape[0] // step)(body)


def scale_kernel(occ_ref, vir_ref, occ_decay_ref, vir_decay_ref, occ_out, vir_out):
    scale_rows(occ_ref, occ_decay_ref, occ_out)
    scale_rows(vir_ref, vir_decay_ref, vir_out)


def scaled(occ, vir, occ_decay, vir_decay):
    shape = jax.ShapeDtypeStruct((occ_decay.shape[0], *occ.shape), jnp.bfloat16)
    return pl.pallas_call(
        scale_kernel,
        out_shape=(shape, shape),
        in_specs=[VMEM] * 4,
        out_specs=(VMEM, VMEM),
        compiler_params=pltpu.CompilerParams(vmem_limit_bytes=12 * MIB),
        cost_estimate=cost(1e8),
    )(occ, vir, occ_decay, vir_decay)


def mark_kernel(cos_ref, kept_ref, planes_ref, cos_out, kept_out):
    z, yl, c, yh, x = (lax.axis_index(name) for name in AXES)
    count = kept_ref.shape[0]
    half = kept_out.shape[1] // 2
    plane = planes_ref[(yh * NX + x) * NZ + z]
    for i, row_yl in enumerate((yl, 1 - yl)):
        row = (z * NYL + row_yl) * NC + c
        for j, from_c in enumerate((c, 1 - c)):
            block = (plane * NYL + yl) * NC + from_c
            kept = kept_ref[(block - row + count) % count].astype(jnp.float32)
            kept_out[i : i + 1, j * half : (j + 1) * half] = jnp.full((1, half), kept, jnp.float32)
    for i in range(cos_out.shape[0]):
        cos_out[i : i + 1, :] = jnp.full((1, cos_out.shape[1]), cos_ref[i], jnp.float32)


def marked(cosine, kept, planes, points):
    return pl.pallas_call(
        mark_kernel,
        out_shape=(
            jax.ShapeDtypeStruct((cosine.shape[0], points), jnp.float32),
            jax.ShapeDtypeStruct((8, 2 * points), jnp.float32),
        ),
        in_specs=[SMEM] * 3,
        out_specs=(VMEM, VMEM),
        compiler_params=pltpu.CompilerParams(vmem_limit_bytes=2 * MIB),
        cost_estimate=cost(1e6),
    )(cosine, kept, planes)


CONTRACT = (((1,), (1,)), ((), ()))


def green(scaled_ref, tile, s_ref):
    taus, _, states = scaled_ref.shape
    rows = pl.ds(pl.multiple_of(tile * TILE, TILE), TILE)
    left = scaled_ref[:, rows, :].reshape(taus * TILE, states)
    return lax.dot_general(left, s_ref[...], CONTRACT, preferred_element_type=jnp.float32)


def occ_kernel(own_ref, near_ref, s_own, s_other, out_ref):
    tiles = own_ref.shape[1] // TILE
    points = s_own.shape[0]
    for i, source in enumerate((own_ref, near_ref)):

        def body(t, i=i, source=source):
            for j, s_ref in enumerate((s_own, s_other)):
                out_ref[i * tiles + t, :, j * points : (j + 1) * points] = green(source, t, s_ref)

        pl.loop(0, tiles)(body)


def occ_term(own, near, s_own, s_other):
    taus, points, states = own.shape
    return pl.pallas_call(
        occ_kernel,
        out_shape=jax.ShapeDtypeStruct((2 * points // TILE, taus * TILE, 2 * points), jnp.float32),
        in_specs=[VMEM] * 4,
        out_specs=VMEM,
        compiler_params=pltpu.CompilerParams(vmem_limit_bytes=26 * MIB),
        cost_estimate=cost(8 * taus * points * points * states),
    )(own, near, s_own, s_other)


def chi_kernel(first, row, cos_ref, kept_ref, scaled_ref, s_own, s_other, occ_ref, out_ref):
    taus, points, _ = scaled_ref.shape

    def body(t):
        rows = pl.ds(pl.multiple_of(t * TILE, TILE), TILE)
        for j, s_ref in enumerate((s_own, s_other)):
            here = slice(j * points, (j + 1) * points)
            product = green(scaled_ref, t, s_ref) * occ_ref[first + t, :, here]
            product = product.reshape(taus, TILE, points)
            for w in range(2):
                chi = cos_ref[w * taus : w * taus + 1, :] * product[0]
                for k in range(1, taus):
                    chi = chi + cos_ref[w * taus + k : w * taus + k + 1, :] * product[k]
                chi = chi * kept_ref[row : row + 1, here]
                high = chi.astype(jnp.bfloat16)
                out_ref[w, 0, rows, here] = high
                out_ref[w, 1, rows, here] = (chi - high.astype(jnp.float32)).astype(jnp.bfloat16)

    pl.loop(0, points // TILE)(body)


def chi_term(row, cos_rows, marks, vir_scaled, s_own, s_other, green_occ):
    taus, points, states = vir_scaled.shape

    def kernel(*refs):
        chi_kernel(row * (points // TILE), row, *refs)

    return pl.pallas_call(
        kernel,
        out_shape=jax.ShapeDtypeStruct((2, 2, points, 2 * points), jnp.bfloat16),
        in_specs=[VMEM] * 6,
        out_specs=VMEM,
        compiler_params=pltpu.CompilerParams(vmem_limit_bytes=24 * MIB),
        cost_estimate=cost(4 * taus * points * points * states),
    )(cos_rows, marks, vir_scaled, s_own, s_other, green_occ)


def answer_kernel(own_ref, near_ref, s_own, s_other, out_ref):
    yl = lax.axis_index("yl")
    points = s_own.shape[0]
    _, groups, _, width, _ = out_ref.shape
    for slot, chi_ref in ((yl, own_ref), (1 - yl, near_ref)):
        for w in range(2):
            both = chi_ref[w].reshape(2 * points, 2 * points)
            answer = jnp.dot(both[:, :points], s_own[...], preferred_element_type=jnp.float32)
            answer = answer + jnp.dot(both[:, points:], s_other[...], preferred_element_type=jnp.float32)
            answer = answer[:points] + answer[points:]
            out_ref[slot, :, w] = answer.T.astype(jnp.bfloat16).reshape(groups, width, points)


def answer_term(own, near, s_own, s_other):
    points, columns = s_own.shape
    groups = NYH * NX
    return pl.pallas_call(
        answer_kernel,
        out_shape=jax.ShapeDtypeStruct((NYL, groups, 2, columns // groups, points), jnp.bfloat16),
        in_specs=[VMEM] * 4,
        out_specs=VMEM,
        compiler_params=pltpu.CompilerParams(vmem_limit_bytes=16 * MIB),
        cost_estimate=cost(32 * points * points * columns),
    )(own, near, s_own, s_other)


def per_device(
    occ_orbitals,
    virt_orbitals,
    columns,
    occ_energies,
    vir_energies,
    tau_index,
    quad_weights,
    frequencies,
    distance_kept,
):
    points = occ_orbitals.shape[0]
    occ_s = from_plane(occ_orbitals)
    occ_near = from_y(occ_orbitals, 1)
    vir_near = from_y(virt_orbitals, -1)
    vir_s = from_plane(virt_orbitals)
    col_s = from_plane(columns)
    occ_t = from_core(occ_s)
    vir_t = from_core(vir_s)
    col_t = from_core(col_s)

    times = 0.05 * jnp.exp(tau_index.astype(jnp.float32) * jnp.float32(math.log(1.5)))
    cosine = (-quad_weights[None, :] * jnp.cos(frequencies[:, None] * times[None, :])).reshape(-1)
    occ_decay = jnp.exp(occ_energies[None, :] * times[:, None])
    vir_decay = jnp.exp(-vir_energies[None, :] * times[:, None])
    planes = jnp.array(PLANES, jnp.int32).reshape(-1)
    cos_rows, marks = marked(cosine, distance_kept, planes, points)
    occ_own, vir_own = scaled(occ_orbitals, virt_orbitals, occ_decay, vir_decay)
    occ_next, vir_next = scaled(occ_near, vir_near, occ_decay, vir_decay)
    green_occ = occ_term(occ_own, occ_next, occ_s, occ_t)
    chi_own = chi_term(0, cos_rows, marks, vir_own, vir_s, vir_t, green_occ)
    chi_near = chi_term(1, cos_rows, marks, vir_next, vir_s, vir_t, green_occ)
    parts = answer_term(chi_own, chi_near, col_s, col_t)
    parts = parts.reshape(-1, *parts.shape[2:])
    spread = lax.all_to_all(parts, ("yl", "yh", "x"), split_axis=0, concat_axis=0, tiled=True)
    return spread.astype(jnp.float32).sum(axis=0)


def solution(mesh):
    fine = Mesh(mesh.devices.reshape(SIZES), AXES)

    rows = P(("z", "yl", "c"), None)
    return jax.shard_map(
        per_device,
        mesh=fine,
        in_specs=(rows, rows, rows, P(), P(), P(), P(), P(), P()),
        out_specs=P(None, ("yh", "x"), ("z", "yl", "c")),
        check_vma=False,
    )
```

```python
import math

import jax
import jax.numpy as jnp
from jax import lax
from jax.experimental import pallas as pl
from jax.experimental.pallas import tpu as pltpu
from jax.sharding import Mesh, PartitionSpec as P


AXES = ("z", "yl", "c", "yh", "x")
SIZES = (8, 2, 2, 2, 4)
_, NYL, NC, NYH, NX = SIZES
PLANES = (
    (0, 5, 6, 3, 4, 1, 2, 7),
    (1, 3, 7, 5, 2, 0, 4, 6),
    (2, 6, 4, 1, 7, 3, 5, 0),
    (3, 7, 1, 4, 6, 2, 0, 5),
    (4, 1, 2, 7, 0, 5, 6, 3),
    (5, 0, 3, 6, 1, 4, 7, 2),
    (6, 4, 0, 2, 5, 7, 3, 1),
    (7, 2, 5, 0, 3, 6, 1, 4),
)
TILE = 128
VMEM = pl.BlockSpec(memory_space=pltpu.VMEM)
SMEM = pl.BlockSpec(memory_space=pltpu.SMEM)
MIB = 1024 * 1024
FIRST_LIMIT = 14 * MIB


def place(at):
    index = 0
    for value, size in zip(at, SIZES):
        index = index * size + value % size
    return index


def everywhere(at=()):
    if len(at) == len(SIZES):
        return [at]
    return [full for i in range(SIZES[len(at)]) for full in everywhere((*at, i))]


def take(array, source):
    return lax.ppermute(array, AXES, [(place(source(*at)), place(at)) for at in everywhere()])


def from_plane(array):
    return take(array, lambda z, yl, c, yh, x: (PLANES[yh * NX + x][z], yl, c, yh, x))


def from_core(array):
    return take(array, lambda z, yl, c, yh, x: (z, yl, c + 1, yh, x))


def from_y(array, by):
    def source(z, yl, c, yh, x):
        y = (yh * NYL + yl + by) % (NYH * NYL)
        return z, y % NYL, c, y // NYL, x

    return take(array, source)


def cost(flops):
    return pl.CostEstimate(flops=int(flops), bytes_accessed=4 * MIB, transcendentals=0)


def scale_rows(source, decay, out):
    step = 16

    def body(i):
        rows = pl.ds(pl.multiple_of(i * step, step), step)
        values = source[rows, :].astype(jnp.float32)
        for k in range(out.shape[0]):
            out[k, rows, :] = (values * decay[k : k + 1, :]).astype(jnp.bfloat16)

    pl.loop(0, source.shape[0] // step)(body)


def scale_kernel(occ_ref, vir_ref, occ_decay_ref, vir_decay_ref, occ_out, vir_out):
    scale_rows(occ_ref, occ_decay_ref, occ_out)
    scale_rows(vir_ref, vir_decay_ref, vir_out)


def scaled(occ, vir, occ_decay, vir_decay):
    shape = jax.ShapeDtypeStruct((occ_decay.shape[0], *occ.shape), jnp.bfloat16)
    return pl.pallas_call(
        scale_kernel,
        out_shape=(shape, shape),
        in_specs=[VMEM] * 4,
        out_specs=(VMEM, VMEM),
        compiler_params=pltpu.CompilerParams(vmem_limit_bytes=12 * MIB),
        cost_estimate=cost(1e8),
    )(occ, vir, occ_decay, vir_decay)


def plane_of(z, yh, x):
    found = jnp.int32(0)
    for g, row in enumerate(PLANES):
        value = jnp.int32(0)
        for i, plane in enumerate(row):
            value = jnp.where(z == i, plane, value)
        found = jnp.where(yh * NX + x == g, value, found)
    return found


def first_kernel(*refs):
    sources, outs, held, sems = refs[:8], refs[8:14], refs[14:22], refs[22]
    copies = [pltpu.make_async_copy(a, b, sems.at[i]) for i, (a, b) in enumerate(zip(sources, held))]
    for copy in copies:
        copy.start()
    for copy in copies:
        copy.wait()
    occ_ref, vir_ref, occ_energy, vir_energy, tau_ref, weight_ref, freq_ref, kept_ref = held
    occ_out, vir_out, occ_decay, vir_decay, cos_out, kept_out = outs
    z, yl, c, yh, x = (lax.axis_index(name) for name in AXES)
    count = kept_ref.shape[0]
    half = kept_out.shape[1] // 2
    plane = plane_of(z, yh, x)
    for i, row_yl in enumerate((yl, 1 - yl)):
        row = (z * NYL + row_yl) * NC + c
        for j, from_c in enumerate((c, 1 - c)):
            block = (plane * NYL + yl) * NC + from_c
            kept = kept_ref[(block - row + count) % count].astype(jnp.float32)
            kept_out[i : i + 1, j * half : (j + 1) * half] = jnp.full((1, half), kept, jnp.float32)
    taus = tau_ref.shape[0]
    for k in range(taus):
        index = jnp.full((1, 128), tau_ref[k].astype(jnp.float32), jnp.float32)
        time = 0.05 * jnp.exp(index * jnp.float32(math.log(1.5)))
        wide = jnp.concatenate([time] * (occ_energy.shape[1] // 128), axis=1)
        occ_decay[k : k + 1, :] = jnp.exp(occ_energy[...] * wide)
        vir_decay[k : k + 1, :] = jnp.exp(-vir_energy[...] * wide)
        for w in range(2):
            cosine = -weight_ref[k] * jnp.cos(freq_ref[w] * time)
            row = w * taus + k
            cos_out[row : row + 1, :] = jnp.concatenate([cosine] * (cos_out.shape[1] // 128), axis=1)
    scale_rows(occ_ref, occ_decay, occ_out)
    scale_rows(vir_ref, vir_decay, vir_out)


def first_term(occ, vir, occ_energies, vir_energies, tau_index, quad_weights, frequencies, distance_kept):
    taus = tau_index.shape[0]
    points, states = occ.shape
    shape = jax.ShapeDtypeStruct((taus, points, states), jnp.bfloat16)
    decay = jax.ShapeDtypeStruct((taus, states), jnp.float32)
    rows = jax.ShapeDtypeStruct((2 * taus, points), jnp.float32)
    marks = jax.ShapeDtypeStruct((8, 2 * points), jnp.float32)
    operands = (
        occ,
        vir,
        occ_energies.reshape(1, -1),
        vir_energies.reshape(1, -1),
        tau_index,
        quad_weights,
        frequencies,
        distance_kept,
    )
    operands = tuple(pltpu.with_memory_space_constraint(a, pltpu.HBM) for a in operands)
    spaces = [pltpu.VMEM] * 4 + [pltpu.SMEM] * 4
    return pl.pallas_call(
        first_kernel,
        out_shape=(shape, shape, decay, decay, rows, marks),
        in_specs=[pl.BlockSpec(memory_space=pltpu.HBM)] * 8,
        out_specs=(VMEM,) * 6,
        scratch_shapes=[space(a.shape, a.dtype) for space, a in zip(spaces, operands)]
        + [pltpu.SemaphoreType.DMA((8,))],
        compiler_params=pltpu.CompilerParams(vmem_limit_bytes=FIRST_LIMIT),
        cost_estimate=cost(1e8),
    )(*operands)


CONTRACT = (((1,), (1,)), ((), ()))


def green(scaled_ref, tile, s_ref):
    taus, _, states = scaled_ref.shape
    rows = pl.ds(pl.multiple_of(tile * TILE, TILE), TILE)
    left = scaled_ref[:, rows, :].reshape(taus * TILE, states)
    return lax.dot_general(left, s_ref[...], CONTRACT, preferred_element_type=jnp.float32)


def occ_kernel(own_ref, near_ref, s_own, s_other, out_ref):
    tiles = own_ref.shape[1] // TILE
    points = s_own.shape[0]
    for i, source in enumerate((own_ref, near_ref)):

        def body(t, i=i, source=source):
            for j, s_ref in enumerate((s_own, s_other)):
                out_ref[i * tiles + t, :, j * points : (j + 1) * points] = green(source, t, s_ref)

        pl.loop(0, tiles)(body)


def occ_term(own, near, s_own, s_other):
    taus, points, states = own.shape
    return pl.pallas_call(
        occ_kernel,
        out_shape=jax.ShapeDtypeStruct((2 * points // TILE, taus * TILE, 2 * points), jnp.float32),
        in_specs=[VMEM] * 4,
        out_specs=VMEM,
        compiler_params=pltpu.CompilerParams(vmem_limit_bytes=26 * MIB),
        cost_estimate=cost(8 * taus * points * points * states),
    )(own, near, s_own, s_other)


def chi_kernel(first, row, cos_ref, kept_ref, scaled_ref, s_own, s_other, occ_ref, out_ref):
    taus, points, _ = scaled_ref.shape

    def body(t):
        rows = pl.ds(pl.multiple_of(t * TILE, TILE), TILE)
        for j, s_ref in enumerate((s_own, s_other)):
            here = slice(j * points, (j + 1) * points)
            product = green(scaled_ref, t, s_ref) * occ_ref[first + t, :, here]
            product = product.reshape(taus, TILE, points)
            for w in range(2):
                chi = cos_ref[w * taus : w * taus + 1, :] * product[0]
                for k in range(1, taus):
                    chi = chi + cos_ref[w * taus + k : w * taus + k + 1, :] * product[k]
                chi = chi * kept_ref[row : row + 1, here]
                high = chi.astype(jnp.bfloat16)
                out_ref[w, 0, rows, here] = high
                out_ref[w, 1, rows, here] = (chi - high.astype(jnp.float32)).astype(jnp.bfloat16)

    pl.loop(0, points // TILE)(body)


def chi_term(row, cos_rows, marks, vir_scaled, s_own, s_other, green_occ):
    taus, points, states = vir_scaled.shape

    def kernel(*refs):
        chi_kernel(row * (points // TILE), row, *refs)

    return pl.pallas_call(
        kernel,
        out_shape=jax.ShapeDtypeStruct((2, 2, points, 2 * points), jnp.bfloat16),
        in_specs=[VMEM] * 6,
        out_specs=VMEM,
        compiler_params=pltpu.CompilerParams(vmem_limit_bytes=24 * MIB),
        cost_estimate=cost(4 * taus * points * points * states),
    )(cos_rows, marks, vir_scaled, s_own, s_other, green_occ)


def answer_kernel(own_ref, near_ref, s_own, s_other, out_ref):
    yl = lax.axis_index("yl")
    points = s_own.shape[0]
    _, groups, _, width, _ = out_ref.shape
    for slot, chi_ref in ((yl, own_ref), (1 - yl, near_ref)):
        for w in range(2):
            both = chi_ref[w].reshape(2 * points, 2 * points)
            answer = jnp.dot(both[:, :points], s_own[...], preferred_element_type=jnp.float32)
            answer = answer + jnp.dot(both[:, points:], s_other[...], preferred_element_type=jnp.float32)
            answer = answer[:points] + answer[points:]
            out_ref[slot, :, w] = answer.T.astype(jnp.bfloat16).reshape(groups, width, points)


def answer_term(own, near, s_own, s_other):
    points, columns = s_own.shape
    groups = NYH * NX
    return pl.pallas_call(
        answer_kernel,
        out_shape=jax.ShapeDtypeStruct((NYL, groups, 2, columns // groups, points), jnp.bfloat16),
        in_specs=[VMEM] * 4,
        out_specs=VMEM,
        compiler_params=pltpu.CompilerParams(vmem_limit_bytes=16 * MIB),
        cost_estimate=cost(32 * points * points * columns),
    )(own, near, s_own, s_other)


def per_device(
    occ_orbitals,
    virt_orbitals,
    columns,
    occ_energies,
    vir_energies,
    tau_index,
    quad_weights,
    frequencies,
    distance_kept,
):
    occ_s = from_plane(occ_orbitals)
    occ_near = from_y(occ_orbitals, 1)
    vir_near = from_y(virt_orbitals, -1)
    vir_s = from_plane(virt_orbitals)
    col_s = from_plane(columns)
    occ_t = from_core(occ_s)
    vir_t = from_core(vir_s)
    col_t = from_core(col_s)

    occ_own, vir_own, occ_decay, vir_decay, cos_rows, marks = first_term(
        occ_orbitals,
        virt_orbitals,
        occ_energies,
        vir_energies,
        tau_index,
        quad_weights,
        frequencies,
        distance_kept,
    )
    occ_next, vir_next = scaled(occ_near, vir_near, occ_decay, vir_decay)
    green_occ = occ_term(occ_own, occ_next, occ_s, occ_t)
    chi_own = chi_term(0, cos_rows, marks, vir_own, vir_s, vir_t, green_occ)
    chi_near = chi_term(1, cos_rows, marks, vir_next, vir_s, vir_t, green_occ)
    parts = answer_term(chi_own, chi_near, col_s, col_t)
    parts = parts.reshape(-1, *parts.shape[2:])
    spread = lax.all_to_all(parts, ("yl", "yh", "x"), split_axis=0, concat_axis=0, tiled=True)
    return spread.astype(jnp.float32).sum(axis=0)


def solution(mesh):
    fine = Mesh(mesh.devices.reshape(SIZES), AXES)

    rows = P(("z", "yl", "c"), None)
    return jax.shard_map(
        per_device,
        mesh=fine,
        in_specs=(rows, rows, rows, P(), P(), P(), P(), P(), P()),
        out_specs=P(None, ("yh", "x"), ("z", "yl", "c")),
        check_vma=False,
    )
```

```python
import math

import jax
import jax.numpy as jnp
from jax import lax
from jax.experimental import pallas as pl
from jax.experimental.pallas import tpu as pltpu
from jax.sharding import Mesh, PartitionSpec as P


AXES = ("z", "yl", "c", "yh", "x")
SIZES = (8, 2, 2, 2, 4)
_, NYL, NC, NYH, NX = SIZES
PLANES = (
    (0, 5, 6, 3, 4, 1, 2, 7),
    (1, 3, 7, 5, 2, 0, 4, 6),
    (2, 6, 4, 1, 7, 3, 5, 0),
    (3, 7, 1, 4, 6, 2, 0, 5),
    (4, 1, 2, 7, 0, 5, 6, 3),
    (5, 0, 3, 6, 1, 4, 7, 2),
    (6, 4, 0, 2, 5, 7, 3, 1),
    (7, 2, 5, 0, 3, 6, 1, 4),
)
TILE = 128
VMEM = pl.BlockSpec(memory_space=pltpu.VMEM)
SMEM = pl.BlockSpec(memory_space=pltpu.SMEM)
MIB = 1024 * 1024
FIRST_LIMIT = 14 * MIB


def place(at):
    index = 0
    for value, size in zip(at, SIZES):
        index = index * size + value % size
    return index


def everywhere(at=()):
    if len(at) == len(SIZES):
        return [at]
    return [full for i in range(SIZES[len(at)]) for full in everywhere((*at, i))]


def take(array, source):
    return lax.ppermute(array, AXES, [(place(source(*at)), place(at)) for at in everywhere()])


def from_plane(array):
    return take(array, lambda z, yl, c, yh, x: (PLANES[yh * NX + x][z], yl, c, yh, x))


def from_core(array):
    return take(array, lambda z, yl, c, yh, x: (z, yl, c + 1, yh, x))


def from_y(array, by):
    def source(z, yl, c, yh, x):
        y = (yh * NYL + yl + by) % (NYH * NYL)
        return z, y % NYL, c, y // NYL, x

    return take(array, source)


def cost(flops):
    return pl.CostEstimate(flops=int(flops), bytes_accessed=4 * MIB, transcendentals=0)


def scale_rows(source, decay, out):
    step = 16

    def body(i):
        rows = pl.ds(pl.multiple_of(i * step, step), step)
        values = source[rows, :].astype(jnp.float32)
        for k in range(out.shape[0]):
            out[k, rows, :] = (values * decay[k : k + 1, :]).astype(jnp.bfloat16)

    pl.loop(0, source.shape[0] // step)(body)


def scale_kernel(occ_ref, vir_ref, occ_decay_ref, vir_decay_ref, occ_out, vir_out):
    scale_rows(occ_ref, occ_decay_ref, occ_out)
    scale_rows(vir_ref, vir_decay_ref, vir_out)


def scaled(occ, vir, occ_decay, vir_decay):
    shape = jax.ShapeDtypeStruct((occ_decay.shape[0], *occ.shape), jnp.bfloat16)
    return pl.pallas_call(
        scale_kernel,
        out_shape=(shape, shape),
        in_specs=[VMEM] * 4,
        out_specs=(VMEM, VMEM),
        compiler_params=pltpu.CompilerParams(vmem_limit_bytes=12 * MIB),
        cost_estimate=cost(1e8),
    )(occ, vir, occ_decay, vir_decay)


def plane_of(z, yh, x):
    found = jnp.int32(0)
    for g, row in enumerate(PLANES):
        value = jnp.int32(0)
        for i, plane in enumerate(row):
            value = jnp.where(z == i, plane, value)
        found = jnp.where(yh * NX + x == g, value, found)
    return found


def first_kernel(*refs):
    sources, outs, held, sems = refs[:8], refs[8:14], refs[14:22], refs[22]
    copies = [pltpu.make_async_copy(a, b, sems.at[i]) for i, (a, b) in enumerate(zip(sources, held))]
    for copy in copies:
        copy.start()
    for copy in copies:
        copy.wait()
    occ_ref, vir_ref, occ_energy, vir_energy, tau_ref, weight_ref, freq_ref, kept_ref = held
    occ_out, vir_out, occ_decay, vir_decay, cos_out, kept_out = outs
    z, yl, c, yh, x = (lax.axis_index(name) for name in AXES)
    count = kept_ref.shape[0]
    half = kept_out.shape[1] // 2
    plane = plane_of(z, yh, x)
    for i, row_yl in enumerate((yl, 1 - yl)):
        row = (z * NYL + row_yl) * NC + c
        for j, from_c in enumerate((c, 1 - c)):
            block = (plane * NYL + yl) * NC + from_c
            kept = kept_ref[(block - row + count) % count].astype(jnp.float32)
            kept_out[i : i + 1, j * half : (j + 1) * half] = jnp.full((1, half), kept, jnp.float32)
    taus = tau_ref.shape[0]
    for k in range(taus):
        index = jnp.full((1, 128), tau_ref[k].astype(jnp.float32), jnp.float32)
        time = 0.05 * jnp.exp(index * jnp.float32(math.log(1.5)))
        wide = jnp.concatenate([time] * (occ_energy.shape[1] // 128), axis=1)
        occ_decay[k : k + 1, :] = jnp.exp(occ_energy[...] * wide)
        vir_decay[k : k + 1, :] = jnp.exp(-vir_energy[...] * wide)
        for w in range(2):
            cosine = -weight_ref[k] * jnp.cos(freq_ref[w] * time)
            row = w * taus + k
            cos_out[row : row + 1, :] = jnp.concatenate([cosine] * (cos_out.shape[1] // 128), axis=1)
    scale_rows(occ_ref, occ_decay, occ_out)
    scale_rows(vir_ref, vir_decay, vir_out)


def first_term(occ, vir, occ_energies, vir_energies, tau_index, quad_weights, frequencies, distance_kept):
    taus = tau_index.shape[0]
    points, states = occ.shape
    shape = jax.ShapeDtypeStruct((taus, points, states), jnp.bfloat16)
    decay = jax.ShapeDtypeStruct((taus, states), jnp.float32)
    rows = jax.ShapeDtypeStruct((2 * taus, points), jnp.float32)
    marks = jax.ShapeDtypeStruct((8, 2 * points), jnp.float32)
    operands = (
        occ,
        vir,
        occ_energies.reshape(1, -1),
        vir_energies.reshape(1, -1),
        tau_index,
        quad_weights,
        frequencies,
        distance_kept,
    )
    operands = tuple(pltpu.with_memory_space_constraint(a, pltpu.HBM) for a in operands)
    spaces = [pltpu.VMEM] * 4 + [pltpu.SMEM] * 4
    return pl.pallas_call(
        first_kernel,
        out_shape=(shape, shape, decay, decay, rows, marks),
        in_specs=[pl.BlockSpec(memory_space=pltpu.HBM)] * 8,
        out_specs=(VMEM,) * 6,
        scratch_shapes=[space(a.shape, a.dtype) for space, a in zip(spaces, operands)]
        + [pltpu.SemaphoreType.DMA((8,))],
        compiler_params=pltpu.CompilerParams(vmem_limit_bytes=FIRST_LIMIT),
        cost_estimate=cost(1e8),
    )(*operands)


CONTRACT = (((1,), (1,)), ((), ()))


def green(scaled_ref, tile, s_ref):
    taus, _, states = scaled_ref.shape
    rows = pl.ds(pl.multiple_of(tile * TILE, TILE), TILE)
    left = scaled_ref[:, rows, :].reshape(taus * TILE, states)
    return lax.dot_general(left, s_ref[...], CONTRACT, preferred_element_type=jnp.float32)


def occ_kernel(own_ref, near_ref, s_own, s_other, out_ref):
    tiles = own_ref.shape[1] // TILE
    points = s_own.shape[0]
    for i, source in enumerate((own_ref, near_ref)):

        def body(t, i=i, source=source):
            for j, s_ref in enumerate((s_own, s_other)):
                out_ref[i * tiles + t, :, j * points : (j + 1) * points] = green(source, t, s_ref)

        pl.loop(0, tiles)(body)


def occ_term(own, near, s_own, s_other):
    taus, points, states = own.shape
    return pl.pallas_call(
        occ_kernel,
        out_shape=jax.ShapeDtypeStruct((2 * points // TILE, taus * TILE, 2 * points), jnp.float32),
        in_specs=[VMEM] * 4,
        out_specs=VMEM,
        compiler_params=pltpu.CompilerParams(vmem_limit_bytes=26 * MIB),
        cost_estimate=cost(8 * taus * points * points * states),
    )(own, near, s_own, s_other)


def chi_kernel(part, cos_ref, kept_ref, own_ref, near_ref, s_ref, occ_ref, out_ref):
    taus, points, _ = own_ref.shape
    tiles = points // TILE
    here = slice(part * points, (part + 1) * points)
    for i, source in enumerate((own_ref, near_ref)):

        def body(t, i=i, source=source):
            rows = pl.ds(pl.multiple_of(i * points + t * TILE, TILE), TILE)
            product = green(source, t, s_ref) * occ_ref[i * tiles + t, :, here]
            product = product.reshape(taus, TILE, points)
            for w in range(2):
                chi = cos_ref[w * taus : w * taus + 1, :] * product[0]
                for k in range(1, taus):
                    chi = chi + cos_ref[w * taus + k : w * taus + k + 1, :] * product[k]
                chi = chi * kept_ref[i : i + 1, here]
                high = chi.astype(jnp.bfloat16)
                out_ref[w, 0, rows, :] = high
                out_ref[w, 1, rows, :] = (chi - high.astype(jnp.float32)).astype(jnp.bfloat16)

        pl.loop(0, tiles)(body)


def chi_term(part, cos_rows, marks, own, near, s, green_occ):
    taus, points, states = own.shape

    def kernel(*refs):
        chi_kernel(part, *refs)

    return pl.pallas_call(
        kernel,
        out_shape=jax.ShapeDtypeStruct((2, 2, 2 * points, points), jnp.bfloat16),
        in_specs=[VMEM] * 6,
        out_specs=VMEM,
        compiler_params=pltpu.CompilerParams(vmem_limit_bytes=24 * MIB),
        cost_estimate=cost(4 * taus * points * points * states),
    )(cos_rows, marks, own, near, s, green_occ)


def response_kernel(chi_ref, s_ref, out_ref):
    points = s_ref.shape[0]
    for w in range(2):
        both = chi_ref[w].reshape(4 * points, points)
        answer = jnp.dot(both, s_ref[...], preferred_element_type=jnp.float32)
        out_ref[w] = answer[: 2 * points] + answer[2 * points :]


def response_term(chi, s):
    points, columns = s.shape
    return pl.pallas_call(
        response_kernel,
        out_shape=jax.ShapeDtypeStruct((2, 2 * points, columns), jnp.float32),
        in_specs=[VMEM] * 2,
        out_specs=VMEM,
        compiler_params=pltpu.CompilerParams(vmem_limit_bytes=12 * MIB),
        cost_estimate=cost(16 * points * points * columns),
    )(chi, s)


def answer_kernel(chi_ref, s_ref, carried_ref, out_ref):
    yl = lax.axis_index("yl")
    points = s_ref.shape[0]
    _, groups, _, width, _ = out_ref.shape
    for w in range(2):
        both = chi_ref[w].reshape(4 * points, points)
        answer = jnp.dot(both, s_ref[...], preferred_element_type=jnp.float32)
        answer = answer[: 2 * points] + answer[2 * points :] + carried_ref[w]
        for slot, part in ((yl, answer[:points]), (1 - yl, answer[points:])):
            out_ref[slot, :, w] = part.T.astype(jnp.bfloat16).reshape(groups, width, points)


def answer_term(chi, s, carried):
    points, columns = s.shape
    groups = NYH * NX
    return pl.pallas_call(
        answer_kernel,
        out_shape=jax.ShapeDtypeStruct((NYL, groups, 2, columns // groups, points), jnp.bfloat16),
        in_specs=[VMEM] * 3,
        out_specs=VMEM,
        compiler_params=pltpu.CompilerParams(vmem_limit_bytes=16 * MIB),
        cost_estimate=cost(16 * points * points * columns),
    )(chi, s, carried)


def per_device(
    occ_orbitals,
    virt_orbitals,
    columns,
    occ_energies,
    vir_energies,
    tau_index,
    quad_weights,
    frequencies,
    distance_kept,
):
    occ_s = from_plane(occ_orbitals)
    occ_near = from_y(occ_orbitals, 1)
    vir_near = from_y(virt_orbitals, -1)
    vir_s = from_plane(virt_orbitals)
    col_s = from_plane(columns)
    occ_t = from_core(occ_s)
    vir_t = from_core(vir_s)
    col_t = from_core(col_s)

    occ_own, vir_own, occ_decay, vir_decay, cos_rows, marks = first_term(
        occ_orbitals,
        virt_orbitals,
        occ_energies,
        vir_energies,
        tau_index,
        quad_weights,
        frequencies,
        distance_kept,
    )
    occ_next, vir_next = scaled(occ_near, vir_near, occ_decay, vir_decay)
    green_occ = occ_term(occ_own, occ_next, occ_s, occ_t)
    chi_s = chi_term(0, cos_rows, marks, vir_own, vir_next, vir_s, green_occ)
    chi_t = chi_term(1, cos_rows, marks, vir_own, vir_next, vir_t, green_occ)
    carried = response_term(chi_s, col_s)
    parts = answer_term(chi_t, col_t, carried)
    parts = parts.reshape(-1, *parts.shape[2:])
    spread = lax.all_to_all(parts, ("yl", "yh", "x"), split_axis=0, concat_axis=0, tiled=True)
    return spread.astype(jnp.float32).sum(axis=0)


def solution(mesh):
    fine = Mesh(mesh.devices.reshape(SIZES), AXES)

    rows = P(("z", "yl", "c"), None)
    return jax.shard_map(
        per_device,
        mesh=fine,
        in_specs=(rows, rows, rows, P(), P(), P(), P(), P(), P()),
        out_specs=P(None, ("yh", "x"), ("z", "yl", "c")),
        check_vma=False,
    )
```

```python
import math

import jax
import jax.numpy as jnp
from jax import lax
from jax.experimental import pallas as pl
from jax.experimental.pallas import tpu as pltpu
from jax.sharding import Mesh, PartitionSpec as P


AXES = ("z", "yl", "c", "yh", "x")
SIZES = (8, 2, 2, 2, 4)
_, NYL, NC, NYH, NX = SIZES
PLANES = (
    (0, 5, 6, 3, 4, 1, 2, 7),
    (1, 3, 7, 5, 2, 0, 4, 6),
    (2, 6, 4, 1, 7, 3, 5, 0),
    (3, 7, 1, 4, 6, 2, 0, 5),
    (4, 1, 2, 7, 0, 5, 6, 3),
    (5, 0, 3, 6, 1, 4, 7, 2),
    (6, 4, 0, 2, 5, 7, 3, 1),
    (7, 2, 5, 0, 3, 6, 1, 4),
)
TILE = 128
VMEM = pl.BlockSpec(memory_space=pltpu.VMEM)
SMEM = pl.BlockSpec(memory_space=pltpu.SMEM)
MIB = 1024 * 1024


def place(at):
    index = 0
    for value, size in zip(at, SIZES):
        index = index * size + value % size
    return index


def everywhere(at=()):
    if len(at) == len(SIZES):
        return [at]
    return [full for i in range(SIZES[len(at)]) for full in everywhere((*at, i))]


def take(array, source):
    return lax.ppermute(array, AXES, [(place(source(*at)), place(at)) for at in everywhere()])


def from_plane(array):
    return take(array, lambda z, yl, c, yh, x: (PLANES[yh * NX + x][z], yl, c, yh, x))


def from_core(array):
    return take(array, lambda z, yl, c, yh, x: (z, yl, c + 1, yh, x))


def from_y(array, by):
    def source(z, yl, c, yh, x):
        y = (yh * NYL + yl + by) % (NYH * NYL)
        return z, y % NYL, c, y // NYL, x

    return take(array, source)


def cost(flops):
    return pl.CostEstimate(flops=int(flops), bytes_accessed=4 * MIB, transcendentals=0)


def scale_rows(source, decay, out):
    step = 16

    def body(i):
        rows = pl.ds(pl.multiple_of(i * step, step), step)
        values = source[rows, :].astype(jnp.float32)
        for k in range(out.shape[0]):
            out[k, rows, :] = (values * decay[k : k + 1, :]).astype(jnp.bfloat16)

    pl.loop(0, source.shape[0] // step)(body)


def scale_kernel(decay_ref, *refs):
    half = len(refs) // 2
    for source, out in zip(refs[:half], refs[half:]):
        scale_rows(source, decay_ref, out)


def scaled(decay, *arrays):
    return pl.pallas_call(
        scale_kernel,
        out_shape=[jax.ShapeDtypeStruct((decay.shape[0], *a.shape), jnp.bfloat16) for a in arrays],
        in_specs=[VMEM] * (1 + len(arrays)),
        out_specs=[VMEM] * len(arrays),
        compiler_params=pltpu.CompilerParams(vmem_limit_bytes=12 * MIB),
        cost_estimate=cost(1e8),
    )(decay, *arrays)


def plane_of(z, yh, x):
    found = jnp.int32(0)
    for g, row in enumerate(PLANES):
        value = jnp.int32(0)
        for i, plane in enumerate(row):
            value = jnp.where(z == i, plane, value)
        found = jnp.where(yh * NX + x == g, value, found)
    return found


def first_kernel(*refs):
    sources, outs, held, sems = refs[:8], refs[8:14], refs[14:21], refs[21]
    held = (*held, outs[-1])
    copies = [pltpu.make_async_copy(a, b, sems.at[i]) for i, (a, b) in enumerate(zip(sources, held))]
    for copy in copies:
        copy.start()
    for copy in copies:
        copy.wait()
    occ_ref, occ_energy, vir_energy, tau_ref, weight_ref, freq_ref, kept_ref, _ = held
    occ_out, occ_decay, vir_decay, cos_out, kept_out, _ = outs
    z, yl, c, yh, x = (lax.axis_index(name) for name in AXES)
    count = kept_ref.shape[0]
    half = kept_out.shape[1] // 2
    plane = plane_of(z, yh, x)
    for i, row_yl in enumerate((yl, 1 - yl)):
        row = (z * NYL + row_yl) * NC + c
        for j, from_c in enumerate((c, 1 - c)):
            block = (plane * NYL + yl) * NC + from_c
            kept = kept_ref[(block - row + count) % count].astype(jnp.float32)
            kept_out[i : i + 1, j * half : (j + 1) * half] = jnp.full((1, half), kept, jnp.float32)
    taus = tau_ref.shape[0]
    for k in range(taus):
        index = jnp.full((1, 128), tau_ref[k].astype(jnp.float32), jnp.float32)
        time = 0.05 * jnp.exp(index * jnp.float32(math.log(1.5)))
        wide = jnp.concatenate([time] * (occ_energy.shape[1] // 128), axis=1)
        occ_decay[k : k + 1, :] = jnp.exp(occ_energy[...] * wide)
        vir_decay[k : k + 1, :] = jnp.exp(-vir_energy[...] * wide)
        for w in range(2):
            cosine = -weight_ref[k] * jnp.cos(freq_ref[w] * time)
            row = w * taus + k
            cos_out[row : row + 1, :] = jnp.concatenate([cosine] * (cos_out.shape[1] // 128), axis=1)
    scale_rows(occ_ref, occ_decay, occ_out)


def first_term(occ, vir, occ_energies, vir_energies, tau_index, quad_weights, frequencies, distance_kept):
    taus = tau_index.shape[0]
    points, states = occ.shape
    decay = jax.ShapeDtypeStruct((taus, states), jnp.float32)
    operands = (
        occ,
        occ_energies.reshape(1, -1),
        vir_energies.reshape(1, -1),
        tau_index,
        quad_weights,
        frequencies,
        distance_kept,
        vir,
    )
    operands = tuple(pltpu.with_memory_space_constraint(a, pltpu.HBM) for a in operands)
    spaces = [pltpu.VMEM] * 3 + [pltpu.SMEM] * 4
    return pl.pallas_call(
        first_kernel,
        out_shape=(
            jax.ShapeDtypeStruct((taus, points, states), jnp.bfloat16),
            decay,
            decay,
            jax.ShapeDtypeStruct((2 * taus, points), jnp.float32),
            jax.ShapeDtypeStruct((8, 2 * points), jnp.float32),
            jax.ShapeDtypeStruct(vir.shape, vir.dtype),
        ),
        in_specs=[pl.BlockSpec(memory_space=pltpu.HBM)] * 8,
        out_specs=(VMEM,) * 6,
        scratch_shapes=[space(a.shape, a.dtype) for space, a in zip(spaces, operands)]
        + [pltpu.SemaphoreType.DMA((8,))],
        compiler_params=pltpu.CompilerParams(vmem_limit_bytes=14 * MIB),
        cost_estimate=cost(1e8),
    )(*operands)


CONTRACT = (((1,), (1,)), ((), ()))


def green(scaled_ref, tile, s_ref):
    taus, _, states = scaled_ref.shape
    rows = pl.ds(tile * TILE, TILE)
    left = scaled_ref[:, rows, :].reshape(taus * TILE, states)
    return lax.dot_general(left, s_ref[...], CONTRACT, preferred_element_type=jnp.float32)


def occ_kernel(own_ref, near_ref, s_own, s_other, out_ref):
    tiles = own_ref.shape[1] // TILE
    points = s_own.shape[0]
    for i, source in enumerate((own_ref, near_ref)):

        def body(t, i=i, source=source):
            for j, s_ref in enumerate((s_own, s_other)):
                out_ref[i * tiles + t, :, j * points : (j + 1) * points] = green(source, t, s_ref)

        for t in range(tiles):
            body(t)


def occ_term(own, near, s_own, s_other):
    taus, points, states = own.shape
    return pl.pallas_call(
        occ_kernel,
        out_shape=jax.ShapeDtypeStruct((2 * points // TILE, taus * TILE, 2 * points), jnp.float32),
        in_specs=[VMEM] * 4,
        out_specs=VMEM,
        compiler_params=pltpu.CompilerParams(vmem_limit_bytes=26 * MIB),
        cost_estimate=cost(8 * taus * points * points * states),
    )(own, near, s_own, s_other)


def chi_kernel(part, cos_ref, kept_ref, own_ref, near_ref, s_ref, occ_ref, out_ref):
    taus, points, _ = own_ref.shape
    tiles = points // TILE
    here = slice(part * points, (part + 1) * points)
    for i, source in enumerate((own_ref, near_ref)):

        def body(t, i=i, source=source):
            rows = pl.ds(i * points + t * TILE, TILE)
            product = green(source, t, s_ref) * occ_ref[i * tiles + t, :, here]
            product = product.reshape(taus, TILE, points)
            for w in range(2):
                chi = cos_ref[w * taus : w * taus + 1, :] * product[0]
                for k in range(1, taus):
                    chi = chi + cos_ref[w * taus + k : w * taus + k + 1, :] * product[k]
                chi = chi * kept_ref[i : i + 1, here]
                high = chi.astype(jnp.bfloat16)
                out_ref[w, 0, rows, :] = high
                out_ref[w, 1, rows, :] = (chi - high.astype(jnp.float32)).astype(jnp.bfloat16)

        for t in range(tiles):
            body(t)


def chi_term(part, cos_rows, marks, own, near, s, green_occ):
    taus, points, states = own.shape

    def kernel(*refs):
        chi_kernel(part, *refs)

    return pl.pallas_call(
        kernel,
        out_shape=jax.ShapeDtypeStruct((2, 2, 2 * points, points), jnp.bfloat16),
        in_specs=[VMEM] * 6,
        out_specs=VMEM,
        compiler_params=pltpu.CompilerParams(vmem_limit_bytes=24 * MIB),
        cost_estimate=cost(4 * taus * points * points * states),
    )(cos_rows, marks, own, near, s, green_occ)


def answer_kernel(chi_ref, chi_other, s_ref, s_other, out_ref):
    yl = lax.axis_index("yl")
    points = s_ref.shape[0]
    _, groups, _, width, _ = out_ref.shape
    for w in range(2):
        both = chi_ref[w].reshape(4 * points, points)
        answer = jnp.dot(both, s_ref[...], preferred_element_type=jnp.float32)
        both = chi_other[w].reshape(4 * points, points)
        answer = answer + jnp.dot(both, s_other[...], preferred_element_type=jnp.float32)
        answer = answer[: 2 * points] + answer[2 * points :]
        for slot, part in ((yl, answer[:points]), (1 - yl, answer[points:])):
            out_ref[slot, :, w] = part.T.astype(jnp.bfloat16).reshape(groups, width, points)


def answer_term(chi, chi_other, s, s_other):
    points, columns = s.shape
    groups = NYH * NX
    return pl.pallas_call(
        answer_kernel,
        out_shape=jax.ShapeDtypeStruct((NYL, groups, 2, columns // groups, points), jnp.bfloat16),
        in_specs=[VMEM] * 4,
        out_specs=VMEM,
        compiler_params=pltpu.CompilerParams(vmem_limit_bytes=16 * MIB),
        cost_estimate=cost(32 * points * points * columns),
    )(chi, chi_other, s, s_other)


def per_device(
    occ_orbitals,
    virt_orbitals,
    columns,
    occ_energies,
    vir_energies,
    tau_index,
    quad_weights,
    frequencies,
    distance_kept,
):
    occ_s = from_plane(occ_orbitals)
    occ_near = from_y(occ_orbitals, 1)
    vir_near = from_y(virt_orbitals, -1)
    vir_s = from_plane(virt_orbitals)
    col_s = from_plane(columns)
    occ_t = from_core(occ_s)
    vir_t = from_core(vir_s)
    col_t = from_core(col_s)

    occ_own, occ_decay, vir_decay, cos_rows, marks, vir_held = first_term(
        occ_orbitals,
        virt_orbitals,
        occ_energies,
        vir_energies,
        tau_index,
        quad_weights,
        frequencies,
        distance_kept,
    )
    (occ_next,) = scaled(occ_decay, occ_near)
    green_occ = occ_term(occ_own, occ_next, occ_s, occ_t)
    vir_near, green_occ = lax.optimization_barrier((vir_near, green_occ))
    vir_own, vir_next = scaled(vir_decay, vir_held, vir_near)
    chi_s = chi_term(0, cos_rows, marks, vir_own, vir_next, vir_s, green_occ)
    chi_t = chi_term(1, cos_rows, marks, vir_own, vir_next, vir_t, green_occ)
    parts = answer_term(chi_s, chi_t, col_s, col_t)
    parts = parts.reshape(-1, *parts.shape[2:])
    spread = lax.all_to_all(parts, ("yl", "yh", "x"), split_axis=0, concat_axis=0, tiled=True)
    return spread.astype(jnp.float32).sum(axis=0)


def solution(mesh):
    fine = Mesh(mesh.devices.reshape(SIZES), AXES)

    rows = P(("z", "yl", "c"), None)
    return jax.shard_map(
        per_device,
        mesh=fine,
        in_specs=(rows, rows, rows, P(), P(), P(), P(), P(), P()),
        out_specs=P(None, ("yh", "x"), ("z", "yl", "c")),
        check_vma=False,
    )
```

```python
import math

import jax
import jax.numpy as jnp
from jax import lax
from jax.experimental import pallas as pl
from jax.experimental.pallas import tpu as pltpu
from jax.sharding import Mesh, PartitionSpec as P


AXES = ("z", "yl", "c", "yh", "x")
SIZES = (8, 2, 2, 2, 4)
_, NYL, NC, NYH, NX = SIZES
PLANES = (
    (0, 5, 6, 3, 4, 1, 2, 7),
    (1, 3, 7, 5, 2, 0, 4, 6),
    (2, 6, 4, 1, 7, 3, 5, 0),
    (3, 7, 1, 4, 6, 2, 0, 5),
    (4, 1, 2, 7, 0, 5, 6, 3),
    (5, 0, 3, 6, 1, 4, 7, 2),
    (6, 4, 0, 2, 5, 7, 3, 1),
    (7, 2, 5, 0, 3, 6, 1, 4),
)
TILE = 128
VMEM = pl.BlockSpec(memory_space=pltpu.VMEM)
SMEM = pl.BlockSpec(memory_space=pltpu.SMEM)
MIB = 1024 * 1024


def place(at):
    index = 0
    for value, size in zip(at, SIZES):
        index = index * size + value % size
    return index


def everywhere(at=()):
    if len(at) == len(SIZES):
        return [at]
    return [full for i in range(SIZES[len(at)]) for full in everywhere((*at, i))]


def take(array, source):
    return lax.ppermute(array, AXES, [(place(source(*at)), place(at)) for at in everywhere()])


def from_plane(array):
    return take(array, lambda z, yl, c, yh, x: (PLANES[yh * NX + x][z], yl, c, yh, x))


def from_core(array):
    return take(array, lambda z, yl, c, yh, x: (z, yl, c + 1, yh, x))


def from_y(array, by):
    def source(z, yl, c, yh, x):
        y = (yh * NYL + yl + by) % (NYH * NYL)
        return z, y % NYL, c, y // NYL, x

    return take(array, source)


def cost(flops):
    return pl.CostEstimate(flops=int(flops), bytes_accessed=4 * MIB, transcendentals=0)


def scale_rows(source, decay, out):
    step = 16

    def body(i):
        rows = pl.ds(pl.multiple_of(i * step, step), step)
        values = source[rows, :].astype(jnp.float32)
        for k in range(out.shape[0]):
            out[k, rows, :] = (values * decay[k : k + 1, :]).astype(jnp.bfloat16)

    pl.loop(0, source.shape[0] // step)(body)


def scale_kernel(decay_ref, *refs):
    half = len(refs) // 2
    for source, out in zip(refs[:half], refs[half:]):
        scale_rows(source, decay_ref, out)


def scaled(decay, *arrays):
    return pl.pallas_call(
        scale_kernel,
        out_shape=[jax.ShapeDtypeStruct((decay.shape[0], *a.shape), jnp.bfloat16) for a in arrays],
        in_specs=[VMEM] * (1 + len(arrays)),
        out_specs=[VMEM] * len(arrays),
        compiler_params=pltpu.CompilerParams(vmem_limit_bytes=12 * MIB),
        cost_estimate=cost(1e8),
    )(decay, *arrays)


def plane_of(z, yh, x):
    found = jnp.int32(0)
    for g, row in enumerate(PLANES):
        value = jnp.int32(0)
        for i, plane in enumerate(row):
            value = jnp.where(z == i, plane, value)
        found = jnp.where(yh * NX + x == g, value, found)
    return found


def first_kernel(*refs):
    sources, outs, held, sems = refs[:8], refs[8:14], refs[14:21], refs[21]
    held = (*held, outs[-1])
    copies = [pltpu.make_async_copy(a, b, sems.at[i]) for i, (a, b) in enumerate(zip(sources, held))]
    for copy in copies:
        copy.start()
    for copy in copies:
        copy.wait()
    occ_ref, occ_energy, vir_energy, tau_ref, weight_ref, freq_ref, kept_ref, _ = held
    occ_out, occ_decay, vir_decay, cos_out, kept_out, _ = outs
    z, yl, c, yh, x = (lax.axis_index(name) for name in AXES)
    count = kept_ref.shape[0]
    half = kept_out.shape[1] // 2
    plane = plane_of(z, yh, x)
    for i, row_yl in enumerate((yl, 1 - yl)):
        row = (z * NYL + row_yl) * NC + c
        for j, from_c in enumerate((c, 1 - c)):
            block = (plane * NYL + yl) * NC + from_c
            kept = kept_ref[(block - row + count) % count].astype(jnp.float32)
            kept_out[i : i + 1, j * half : (j + 1) * half] = jnp.full((1, half), kept, jnp.float32)
    taus = tau_ref.shape[0]
    for k in range(taus):
        index = jnp.full((1, 128), tau_ref[k].astype(jnp.float32), jnp.float32)
        time = 0.05 * jnp.exp(index * jnp.float32(math.log(1.5)))
        wide = jnp.concatenate([time] * (occ_energy.shape[1] // 128), axis=1)
        occ_decay[k : k + 1, :] = jnp.exp(occ_energy[...] * wide)
        vir_decay[k : k + 1, :] = jnp.exp(-vir_energy[...] * wide)
        for w in range(2):
            cosine = -weight_ref[k] * jnp.cos(freq_ref[w] * time)
            row = w * taus + k
            cos_out[row : row + 1, :] = jnp.concatenate([cosine] * (cos_out.shape[1] // 128), axis=1)
    scale_rows(occ_ref, occ_decay, occ_out)


def first_term(occ, vir, occ_energies, vir_energies, tau_index, quad_weights, frequencies, distance_kept):
    taus = tau_index.shape[0]
    points, states = occ.shape
    decay = jax.ShapeDtypeStruct((taus, states), jnp.float32)
    operands = (
        occ,
        occ_energies.reshape(1, -1),
        vir_energies.reshape(1, -1),
        tau_index,
        quad_weights,
        frequencies,
        distance_kept,
        vir,
    )
    operands = tuple(pltpu.with_memory_space_constraint(a, pltpu.HBM) for a in operands)
    spaces = [pltpu.VMEM] * 3 + [pltpu.SMEM] * 4
    return pl.pallas_call(
        first_kernel,
        out_shape=(
            jax.ShapeDtypeStruct((taus, points, states), jnp.bfloat16),
            decay,
            decay,
            jax.ShapeDtypeStruct((2 * taus, points), jnp.float32),
            jax.ShapeDtypeStruct((8, 2 * points), jnp.float32),
            jax.ShapeDtypeStruct(vir.shape, vir.dtype),
        ),
        in_specs=[pl.BlockSpec(memory_space=pltpu.HBM)] * 8,
        out_specs=(VMEM,) * 6,
        scratch_shapes=[space(a.shape, a.dtype) for space, a in zip(spaces, operands)]
        + [pltpu.SemaphoreType.DMA((8,))],
        compiler_params=pltpu.CompilerParams(vmem_limit_bytes=14 * MIB),
        cost_estimate=cost(1e8),
    )(*operands)


CONTRACT = (((1,), (1,)), ((), ()))


def green(scaled_ref, tile, s_ref):
    taus, _, states = scaled_ref.shape
    rows = pl.ds(tile * TILE, TILE)
    left = scaled_ref[:, rows, :].reshape(taus * TILE, states)
    return lax.dot_general(left, s_ref[...], CONTRACT, preferred_element_type=jnp.float32)


def occ_kernel(own_ref, near_ref, s_own, s_other, out_ref):
    tiles = own_ref.shape[1] // TILE
    points = s_own.shape[0]
    for i, source in enumerate((own_ref, near_ref)):

        def body(t, i=i, source=source):
            for j, s_ref in enumerate((s_own, s_other)):
                out_ref[i * tiles + t, :, j * points : (j + 1) * points] = green(source, t, s_ref)

        for t in range(tiles):
            body(t)


def occ_term(own, near, s_own, s_other):
    taus, points, states = own.shape
    return pl.pallas_call(
        occ_kernel,
        out_shape=jax.ShapeDtypeStruct((2 * points // TILE, taus * TILE, 2 * points), jnp.float32),
        in_specs=[VMEM] * 4,
        out_specs=VMEM,
        compiler_params=pltpu.CompilerParams(vmem_limit_bytes=26 * MIB),
        cost_estimate=cost(8 * taus * points * points * states),
    )(own, near, s_own, s_other)


def chi_kernel(part, rows_of, cos_ref, kept_ref, *refs):
    sources, (s_ref, occ_ref, out_ref) = refs[:-3], refs[-3:]
    taus, points, _ = sources[0].shape
    tiles = points // TILE
    here = slice(part * points, (part + 1) * points)
    for place_at, (i, source) in enumerate(zip(rows_of, sources)):
        for t in range(tiles):
            rows = pl.ds(place_at * points + t * TILE, TILE)
            product = green(source, t, s_ref) * occ_ref[i * tiles + t, :, here]
            product = product.reshape(taus, TILE, points)
            for w in range(2):
                chi = cos_ref[w * taus : w * taus + 1, :] * product[0]
                for k in range(1, taus):
                    chi = chi + cos_ref[w * taus + k : w * taus + k + 1, :] * product[k]
                chi = chi * kept_ref[i : i + 1, here]
                high = chi.astype(jnp.bfloat16)
                out_ref[w, 0, rows, :] = high
                out_ref[w, 1, rows, :] = (chi - high.astype(jnp.float32)).astype(jnp.bfloat16)


def chi_term(part, cos_rows, marks, blocks, s, green_occ):
    taus, points, states = next(iter(blocks.values())).shape

    def kernel(*refs):
        chi_kernel(part, tuple(blocks), *refs)

    return pl.pallas_call(
        kernel,
        out_shape=jax.ShapeDtypeStruct((2, 2, len(blocks) * points, points), jnp.bfloat16),
        in_specs=[VMEM] * (4 + len(blocks)),
        out_specs=VMEM,
        compiler_params=pltpu.CompilerParams(vmem_limit_bytes=24 * MIB),
        cost_estimate=cost(2 * len(blocks) * taus * points * points * states),
    )(cos_rows, marks, *blocks.values(), s, green_occ)


def answer_kernel(chi_ref, own_other, near_other, s_ref, s_other, out_ref):
    yl = lax.axis_index("yl")
    points = s_ref.shape[0]
    _, groups, _, width, _ = out_ref.shape
    for w in range(2):
        both = chi_ref[w].reshape(4 * points, points)
        answer = jnp.dot(both, s_ref[...], preferred_element_type=jnp.float32)
        answer = answer[: 2 * points] + answer[2 * points :]
        for i, (slot, other) in enumerate(((yl, own_other), (1 - yl, near_other))):
            both = other[w].reshape(2 * points, points)
            rest = jnp.dot(both, s_other[...], preferred_element_type=jnp.float32)
            part = answer[i * points : (i + 1) * points] + rest[:points] + rest[points:]
            out_ref[slot, :, w] = part.T.astype(jnp.bfloat16).reshape(groups, width, points)


def answer_term(chi, own_other, near_other, s, s_other):
    points, columns = s.shape
    groups = NYH * NX
    return pl.pallas_call(
        answer_kernel,
        out_shape=jax.ShapeDtypeStruct((NYL, groups, 2, columns // groups, points), jnp.bfloat16),
        in_specs=[VMEM] * 5,
        out_specs=VMEM,
        compiler_params=pltpu.CompilerParams(vmem_limit_bytes=16 * MIB),
        cost_estimate=cost(32 * points * points * columns),
    )(chi, own_other, near_other, s, s_other)


def per_device(
    occ_orbitals,
    virt_orbitals,
    columns,
    occ_energies,
    vir_energies,
    tau_index,
    quad_weights,
    frequencies,
    distance_kept,
):
    occ_s = from_plane(occ_orbitals)
    occ_near = from_y(occ_orbitals, 1)
    vir_near = from_y(virt_orbitals, -1)
    vir_s = from_plane(virt_orbitals)
    col_s = from_plane(columns)
    occ_t = from_core(occ_s)
    vir_t = from_core(vir_s)
    col_t = from_core(col_s)

    occ_own, occ_decay, vir_decay, cos_rows, marks, vir_held = first_term(
        occ_orbitals,
        virt_orbitals,
        occ_energies,
        vir_energies,
        tau_index,
        quad_weights,
        frequencies,
        distance_kept,
    )
    (occ_next,) = scaled(occ_decay, occ_near)
    green_occ = occ_term(occ_own, occ_next, occ_s, occ_t)
    vir_near, green_occ = lax.optimization_barrier((vir_near, green_occ))
    vir_own, vir_next = scaled(vir_decay, vir_held, vir_near)
    chi_s = chi_term(0, cos_rows, marks, {0: vir_own, 1: vir_next}, vir_s, green_occ)
    chi_own = chi_term(1, cos_rows, marks, {0: vir_own}, vir_t, green_occ)
    chi_near = chi_term(1, cos_rows, marks, {1: vir_next}, vir_t, green_occ)
    parts = answer_term(chi_s, chi_own, chi_near, col_s, col_t)
    parts = parts.reshape(-1, *parts.shape[2:])
    spread = lax.all_to_all(parts, ("yl", "yh", "x"), split_axis=0, concat_axis=0, tiled=True)
    return spread.astype(jnp.float32).sum(axis=0)


def solution(mesh):
    fine = Mesh(mesh.devices.reshape(SIZES), AXES)

    rows = P(("z", "yl", "c"), None)
    return jax.shard_map(
        per_device,
        mesh=fine,
        in_specs=(rows, rows, rows, P(), P(), P(), P(), P(), P()),
        out_specs=P(None, ("yh", "x"), ("z", "yl", "c")),
        check_vma=False,
    )
```

```python
import math

import jax
import jax.numpy as jnp
from jax import lax
from jax.experimental import pallas as pl
from jax.experimental.pallas import tpu as pltpu
from jax.sharding import Mesh, PartitionSpec as P


AXES = ("z", "yl", "c", "yh", "x")
SIZES = (8, 2, 2, 2, 4)
_, NYL, NC, NYH, NX = SIZES
PLANES = (
    (0, 5, 6, 3, 4, 1, 2, 7),
    (1, 3, 7, 5, 2, 0, 4, 6),
    (2, 6, 4, 1, 7, 3, 5, 0),
    (3, 7, 1, 4, 6, 2, 0, 5),
    (4, 1, 2, 7, 0, 5, 6, 3),
    (5, 0, 3, 6, 1, 4, 7, 2),
    (6, 4, 0, 2, 5, 7, 3, 1),
    (7, 2, 5, 0, 3, 6, 1, 4),
)
TILE = 128
VMEM = pl.BlockSpec(memory_space=pltpu.VMEM)
SMEM = pl.BlockSpec(memory_space=pltpu.SMEM)
MIB = 1024 * 1024


def place(at):
    index = 0
    for value, size in zip(at, SIZES):
        index = index * size + value % size
    return index


def everywhere(at=()):
    if len(at) == len(SIZES):
        return [at]
    return [full for i in range(SIZES[len(at)]) for full in everywhere((*at, i))]


def take(array, source):
    return lax.ppermute(array, AXES, [(place(source(*at)), place(at)) for at in everywhere()])


def from_plane(array):
    return take(array, lambda z, yl, c, yh, x: (PLANES[yh * NX + x][z], yl, c, yh, x))


def from_core(array):
    return take(array, lambda z, yl, c, yh, x: (z, yl, c + 1, yh, x))


def from_y(array, by):
    def source(z, yl, c, yh, x):
        y = (yh * NYL + yl + by) % (NYH * NYL)
        return z, y % NYL, c, y // NYL, x

    return take(array, source)


def cost(flops):
    return pl.CostEstimate(flops=int(flops), bytes_accessed=4 * MIB, transcendentals=0)


def scale_rows(source, decay, out):
    step = 16

    def body(i):
        rows = pl.ds(pl.multiple_of(i * step, step), step)
        values = source[rows, :].astype(jnp.float32)
        for k in range(out.shape[0]):
            out[k, rows, :] = (values * decay[k : k + 1, :]).astype(jnp.bfloat16)

    pl.loop(0, source.shape[0] // step)(body)


def scale_kernel(decay_ref, *refs):
    half = len(refs) // 2
    for source, out in zip(refs[:half], refs[half:]):
        scale_rows(source, decay_ref, out)


def scaled(decay, *arrays):
    return pl.pallas_call(
        scale_kernel,
        out_shape=[jax.ShapeDtypeStruct((decay.shape[0], *a.shape), jnp.bfloat16) for a in arrays],
        in_specs=[VMEM] * (1 + len(arrays)),
        out_specs=[VMEM] * len(arrays),
        compiler_params=pltpu.CompilerParams(vmem_limit_bytes=12 * MIB),
        cost_estimate=cost(1e8),
    )(decay, *arrays)


def plane_of(z, yh, x):
    found = jnp.int32(0)
    for g, row in enumerate(PLANES):
        value = jnp.int32(0)
        for i, plane in enumerate(row):
            value = jnp.where(z == i, plane, value)
        found = jnp.where(yh * NX + x == g, value, found)
    return found


def first_kernel(*refs):
    sources, outs, held, sems = refs[:8], refs[8:14], refs[14:21], refs[21]
    held = (*held, outs[-1])
    copies = [pltpu.make_async_copy(a, b, sems.at[i]) for i, (a, b) in enumerate(zip(sources, held))]
    for copy in copies:
        copy.start()
    for copy in copies:
        copy.wait()
    occ_ref, occ_energy, vir_energy, tau_ref, weight_ref, freq_ref, kept_ref, _ = held
    occ_out, occ_decay, vir_decay, cos_out, kept_out, _ = outs
    z, yl, c, yh, x = (lax.axis_index(name) for name in AXES)
    count = kept_ref.shape[0]
    half = kept_out.shape[1] // 2
    plane = plane_of(z, yh, x)
    for i, row_yl in enumerate((yl, 1 - yl)):
        row = (z * NYL + row_yl) * NC + c
        for j, from_c in enumerate((c, 1 - c)):
            block = (plane * NYL + yl) * NC + from_c
            kept = kept_ref[(block - row + count) % count].astype(jnp.float32)
            kept_out[i : i + 1, j * half : (j + 1) * half] = jnp.full((1, half), kept, jnp.float32)
    taus = tau_ref.shape[0]
    for k in range(taus):
        index = jnp.full((1, 128), tau_ref[k].astype(jnp.float32), jnp.float32)
        time = 0.05 * jnp.exp(index * jnp.float32(math.log(1.5)))
        wide = jnp.concatenate([time] * (occ_energy.shape[1] // 128), axis=1)
        occ_decay[k : k + 1, :] = jnp.exp(occ_energy[...] * wide)
        vir_decay[k : k + 1, :] = jnp.exp(-vir_energy[...] * wide)
        for w in range(2):
            cosine = -weight_ref[k] * jnp.cos(freq_ref[w] * time)
            row = w * taus + k
            cos_out[row : row + 1, :] = jnp.concatenate([cosine] * (cos_out.shape[1] // 128), axis=1)
    scale_rows(occ_ref, occ_decay, occ_out)


def first_term(occ, vir, occ_energies, vir_energies, tau_index, quad_weights, frequencies, distance_kept):
    taus = tau_index.shape[0]
    points, states = occ.shape
    decay = jax.ShapeDtypeStruct((taus, states), jnp.float32)
    operands = (
        occ,
        occ_energies.reshape(1, -1),
        vir_energies.reshape(1, -1),
        tau_index,
        quad_weights,
        frequencies,
        distance_kept,
        vir,
    )
    operands = tuple(pltpu.with_memory_space_constraint(a, pltpu.HBM) for a in operands)
    spaces = [pltpu.VMEM] * 3 + [pltpu.SMEM] * 4
    return pl.pallas_call(
        first_kernel,
        out_shape=(
            jax.ShapeDtypeStruct((taus, points, states), jnp.bfloat16),
            decay,
            decay,
            jax.ShapeDtypeStruct((2 * taus, points), jnp.float32),
            jax.ShapeDtypeStruct((8, 2 * points), jnp.float32),
            jax.ShapeDtypeStruct(vir.shape, vir.dtype),
        ),
        in_specs=[pl.BlockSpec(memory_space=pltpu.HBM)] * 8,
        out_specs=(VMEM,) * 6,
        scratch_shapes=[space(a.shape, a.dtype) for space, a in zip(spaces, operands)]
        + [pltpu.SemaphoreType.DMA((8,))],
        compiler_params=pltpu.CompilerParams(vmem_limit_bytes=14 * MIB),
        cost_estimate=cost(1e8),
    )(*operands)


CONTRACT = (((1,), (1,)), ((), ()))


def green(scaled_ref, tile, s_ref):
    taus, _, states = scaled_ref.shape
    rows = pl.ds(tile * TILE, TILE)
    left = scaled_ref[:, rows, :].reshape(taus * TILE, states)
    return lax.dot_general(left, s_ref[...], CONTRACT, preferred_element_type=jnp.float32)


def occ_kernel(own_ref, near_ref, s_own, s_other, out_ref):
    tiles = own_ref.shape[1] // TILE
    points = s_own.shape[0]
    for i, source in enumerate((own_ref, near_ref)):

        def body(t, i=i, source=source):
            for j, s_ref in enumerate((s_own, s_other)):
                out_ref[i * tiles + t, :, j * points : (j + 1) * points] = green(source, t, s_ref)

        for t in range(tiles):
            body(t)


def occ_term(own, near, s_own, s_other):
    taus, points, states = own.shape
    return pl.pallas_call(
        occ_kernel,
        out_shape=jax.ShapeDtypeStruct((2 * points // TILE, taus * TILE, 2 * points), jnp.float32),
        in_specs=[VMEM] * 4,
        out_specs=VMEM,
        compiler_params=pltpu.CompilerParams(vmem_limit_bytes=26 * MIB),
        cost_estimate=cost(8 * taus * points * points * states),
    )(own, near, s_own, s_other)


def chi_kernel(part, rows_of, cos_ref, kept_ref, *refs):
    sources, (s_ref, occ_ref, out_ref) = refs[:-3], refs[-3:]
    taus, points, _ = sources[0].shape
    tiles = points // TILE
    here = slice(part * points, (part + 1) * points)
    for place_at, (i, source) in enumerate(zip(rows_of, sources)):
        for t in range(tiles):
            rows = pl.ds(place_at * points + t * TILE, TILE)
            product = green(source, t, s_ref) * occ_ref[i * tiles + t, :, here]
            product = product.reshape(taus, TILE, points)
            for w in range(2):
                chi = cos_ref[w * taus : w * taus + 1, :] * product[0]
                for k in range(1, taus):
                    chi = chi + cos_ref[w * taus + k : w * taus + k + 1, :] * product[k]
                chi = chi * kept_ref[i : i + 1, here]
                high = chi.astype(jnp.bfloat16)
                out_ref[w, 0, rows, :] = high
                out_ref[w, 1, rows, :] = (chi - high.astype(jnp.float32)).astype(jnp.bfloat16)


def chi_term(part, cos_rows, marks, blocks, s, green_occ):
    taus, points, states = next(iter(blocks.values())).shape

    def kernel(*refs):
        chi_kernel(part, tuple(blocks), *refs)

    return pl.pallas_call(
        kernel,
        out_shape=jax.ShapeDtypeStruct((2, 2, len(blocks) * points, points), jnp.bfloat16),
        in_specs=[VMEM] * (4 + len(blocks)),
        out_specs=VMEM,
        compiler_params=pltpu.CompilerParams(vmem_limit_bytes=24 * MIB),
        cost_estimate=cost(2 * len(blocks) * taus * points * points * states),
    )(cos_rows, marks, *blocks.values(), s, green_occ)


def answer_kernel(chi_ref, own_other, near_other, s_ref, s_other, out_ref):
    yl = lax.axis_index("yl")
    points = s_ref.shape[0]
    groups, _, _, width, _ = out_ref.shape
    for w in range(2):
        both = chi_ref[w].reshape(4 * points, points)
        answer = jnp.dot(both, s_ref[...], preferred_element_type=jnp.float32)
        answer = answer[: 2 * points] + answer[2 * points :]
        for i, (slot, other) in enumerate(((yl, own_other), (1 - yl, near_other))):
            both = other[w].reshape(2 * points, points)
            rest = jnp.dot(both, s_other[...], preferred_element_type=jnp.float32)
            part = answer[i * points : (i + 1) * points] + rest[:points] + rest[points:]
            out_ref[:, slot, w] = part.T.astype(jnp.bfloat16).reshape(groups, width, points)


def answer_term(chi, own_other, near_other, s, s_other):
    points, columns = s.shape
    groups = NYH * NX
    return pl.pallas_call(
        answer_kernel,
        out_shape=jax.ShapeDtypeStruct((groups, NYL, 2, columns // groups, points), jnp.bfloat16),
        in_specs=[VMEM] * 5,
        out_specs=VMEM,
        compiler_params=pltpu.CompilerParams(vmem_limit_bytes=16 * MIB),
        cost_estimate=cost(32 * points * points * columns),
    )(chi, own_other, near_other, s, s_other)


def per_device(
    occ_orbitals,
    virt_orbitals,
    columns,
    occ_energies,
    vir_energies,
    tau_index,
    quad_weights,
    frequencies,
    distance_kept,
):
    occ_s = from_plane(occ_orbitals)
    occ_near = from_y(occ_orbitals, 1)
    vir_near = from_y(virt_orbitals, -1)
    vir_s = from_plane(virt_orbitals)
    col_s = from_plane(columns)
    occ_t = from_core(occ_s)
    vir_t = from_core(vir_s)
    col_t = from_core(col_s)

    occ_own, occ_decay, vir_decay, cos_rows, marks, vir_held = first_term(
        occ_orbitals,
        virt_orbitals,
        occ_energies,
        vir_energies,
        tau_index,
        quad_weights,
        frequencies,
        distance_kept,
    )
    (occ_next,) = scaled(occ_decay, occ_near)
    green_occ = occ_term(occ_own, occ_next, occ_s, occ_t)
    vir_near, green_occ = lax.optimization_barrier((vir_near, green_occ))
    vir_own, vir_next = scaled(vir_decay, vir_held, vir_near)
    chi_s = chi_term(0, cos_rows, marks, {0: vir_own, 1: vir_next}, vir_s, green_occ)
    chi_own = chi_term(1, cos_rows, marks, {0: vir_own}, vir_t, green_occ)
    chi_near = chi_term(1, cos_rows, marks, {1: vir_next}, vir_t, green_occ)
    parts = answer_term(chi_s, chi_own, chi_near, col_s, col_t)
    parts = parts.reshape(-1, *parts.shape[2:])
    spread = lax.all_to_all(parts, ("yh", "x", "yl"), split_axis=0, concat_axis=0, tiled=True)
    return spread.astype(jnp.float32).sum(axis=0)


def solution(mesh):
    fine = Mesh(mesh.devices.reshape(SIZES), AXES)

    rows = P(("z", "yl", "c"), None)
    return jax.shard_map(
        per_device,
        mesh=fine,
        in_specs=(rows, rows, rows, P(), P(), P(), P(), P(), P()),
        out_specs=P(None, ("yh", "x"), ("z", "yl", "c")),
        check_vma=False,
    )
```
